32 devices in a mesh: parts: 2 (over x), snp: 16 (over z, y, core).
Axes of the slice: x: 2, y: 2, z: 4, core: 2. Of those that a mesh axis runs over, the one named last changes fastest.
Arguments:
- local_block: float32 [32768, 1024], P(('parts', 'snp')), parts along dimension 0, may hold values from -1 to 1, as said below
- next_block: float32 [32768, 1024], P(('parts', 'snp')), parts along dimension 0, may hold values from -1 to 1, as said below
- shrinkage: float32 [64, 1], replicated, may hold values from 0.3 to 1
- marginal: float32 [64, 32768], P(None, ('parts', 'snp')), parts along dimension 1, may hold values from -12 to 12
- warm_start: float32 [64, 32768], P(None, ('parts', 'snp')), parts along dimension 1, may hold values from -3 to 3
Outputs:
- solution: float32 [64, 32768], P(None, ('parts', 'snp')), parts along dimension 1
- residual: float32 [64, 32768], P(None, ('parts', 'snp')), parts along dimension 1
The draws below stay inside these ranges and needn't reach their ends.
There are 2 independent parts, one for each index of `parts`. The reference program is written for one: setup_inputs(seed, part) draws one part's arguments, and reference() takes and returns one part's arrays. A program takes and returns all parts, laid end to end along the dimension named above; an argument that names none is the same for every part. Nothing has to cross between parts.
Inputs may be any that keep to these rules, and one draw needn't show every extreme that they name: `local_block`: each 1024 x 1024 block of rows is symmetric with ones on its diagonal. `next_block`: inside each 1024 x 1024 block of rows, entries whose column index exceeds the row index are zero; the last block of rows is zero.
All inputs are finite; a program needn't handle non-finite values.
Results may differ from the reference program's by a relative error of at most 0.0003.
Values sent between devices are 32-bit elements; how exact they have to be, the bound alone decides.
No kernel may reach another device: no remote copies, remote signals or barrier semaphores. Data moves between devices by JAX's collectives and lax.ppermute only.
A program may use at most 64 MiB of HBM per device.

```python
import math
import jax
import jax.numpy as jnp
from jax import lax

BLOCK = 1024
TRAITS = 64
ITERS = 3
NSNP = 16384


def draw_local_block(key, part):
    count = NSNP // BLOCK
    half = 0.5 / math.sqrt(2.0 * BLOCK)
    raw = jax.random.uniform(jax.random.fold_in(key, 11), (count, BLOCK, BLOCK), jnp.float32, -half, half)
    sym = (raw + jnp.swapaxes(raw, 1, 2)) * (1.0 / math.sqrt(2.0))
    unit = jnp.eye(BLOCK, dtype=jnp.float32)[None]
    blocks = sym * (1.0 - unit) + unit
    return blocks.reshape(NSNP, BLOCK)


def draw_next_block(key, part):
    count = NSNP // BLOCK
    half = 0.5 / math.sqrt(2.0 * BLOCK)
    raw = jax.random.uniform(jax.random.fold_in(key, 12), (count, BLOCK, BLOCK), jnp.float32, -half, half)
    rows = jnp.arange(BLOCK)[:, None]
    cols = jnp.arange(BLOCK)[None, :]
    lower = (cols <= rows).astype(jnp.float32)[None]
    keep = (jnp.arange(count) < count - 1).astype(jnp.float32)[:, None, None]
    return (raw * lower * keep).reshape(NSNP, BLOCK)


def draw_marginal(key, part):
    noise = jnp.clip(jax.random.normal(jax.random.fold_in(key, 13), (TRAITS, NSNP), jnp.float32), -4.0, 4.0)
    return noise


def block_scale(own_key, shape, split, smallest, top_value):
    loudness, own = 1.0, jax.random.fold_in(own_key, 6)
    for dim, shards_of in split:
        heights = jnp.exp(jax.random.uniform(jax.random.fold_in(own, dim), (shards_of,), jnp.float32, smallest / len(split), top_value / len(split)))
        loudness = loudness * jnp.repeat(heights, shape[dim] // shards_of).reshape([-1 if axis == dim else 1 for axis in range(len(shape))])
    return loudness


def bell_draw(rng, extent, scale, bound, shards=(), kind=jnp.bfloat16):
    array = scale * jax.random.normal(rng, extent, jnp.float32)
    if shards:
        array = array * block_scale(rng, extent, shards, -0.22, 0.18)
    return jnp.clip(array, -bound, bound).astype(kind)


def setup_inputs(seed: int = 0, part: int = 0) -> dict:
    seeds = jax.random.split(jax.random.key(seed), 6)
    part_splits = jax.random.split(jax.random.fold_in(seeds[5], part), 6)
    return {
        "local_block": draw_local_block(jax.random.fold_in(jax.random.fold_in(seeds[5], part), 71), part),
        "next_block": draw_next_block(jax.random.fold_in(jax.random.fold_in(seeds[5], part), 71), part),
        "shrinkage": jnp.clip(jnp.exp(jax.random.uniform(seeds[2], (TRAITS, 1), jnp.float32, math.log(0.3), math.log(1.0))), 0.3, 1.0),
        "marginal": draw_marginal(jax.random.fold_in(jax.random.fold_in(seeds[5], part), 71), part),
        "warm_start": bell_draw(part_splits[4], (TRAITS, NSNP), 0.5, 3.0, ((1, 16),), jnp.float32),
    }


HIGH = lax.Precision.HIGHEST


def operate(field, local_block, next_block, shrinkage):
    traits = field.shape[0]
    count = field.shape[1] // BLOCK
    blocks = field.reshape(traits, count, BLOCK)
    own_blocks = local_block.reshape(count, BLOCK, BLOCK)
    next_blocks = next_block.reshape(count, BLOCK, BLOCK)
    filler = jnp.zeros((traits, 1, BLOCK), field.dtype)
    own = jnp.einsum('tnb,nba->tna', blocks, own_blocks, precision=HIGH)
    upper = jnp.concatenate([blocks[:, 1:], filler], axis=1)
    forward = jnp.einsum('tnb,nab->tna', upper, next_blocks, precision=HIGH)
    backward = jnp.einsum('tnb,nba->tna', blocks, next_blocks, precision=HIGH)
    backward = jnp.concatenate([filler, backward[:, :-1]], axis=1)
    return (own + forward + backward).reshape(traits, count * BLOCK) + shrinkage * field


def reference(local_block, next_block, shrinkage, marginal, warm_start):
    solution = warm_start
    residual = marginal - operate(warm_start, local_block, next_block, shrinkage)
    direction = residual
    norm_now = jnp.sum(residual * residual, axis=1, keepdims=True)
    for step in range(ITERS):
        image = operate(direction, local_block, next_block, shrinkage)
        alpha = norm_now / jnp.sum(direction * image, axis=1, keepdims=True)
        solution = solution + alpha * direction
        residual = residual - alpha * image
        norm_next = jnp.sum(residual * residual, axis=1, keepdims=True)
        direction = residual + (norm_next / norm_now) * direction
        norm_now = norm_next
    return solution, residual
```

```python
import functools

import jax
import jax.numpy as jnp
from jax import lax
from jax.experimental import pallas as pl
from jax.experimental.pallas import tpu as pltpu
from jax.sharding import PartitionSpec as P

ITERS = 3
F32 = jnp.float32
BF16 = jnp.bfloat16
VMEM = pltpu.VMEM
MOMENT_ROWS = 8


def tile_of(size):
    return 256 if size % 256 == 0 else size


def halves(x):
    high = x.astype(BF16)
    return high, (x - high.astype(F32)).astype(BF16)


def dot(left, right, across):
    dims = (((1,), (1 if across else 0,)), ((), ()))
    return lax.dot_general(left, right, dims, preferred_element_type=F32)


def product(both, right_high, right_low, across=False):
    rows = both.shape[0] // 2
    main = dot(both, right_high, across)
    return main[:rows] + main[rows:] + dot(both[:rows], right_low, across)


def stacked(field):
    return jnp.concatenate(halves(field), axis=0)


def coupling(both, high, low, store):
    size = high.shape[0]
    tile = tile_of(size)
    for start in range(0, size, tile):
        rows, cols = pl.ds(start, size - start), pl.ds(start, tile)
        store(start, product(both[:, start:], high[rows, cols], low[rows, cols]))


def forward(both, high, low, store):
    size = high.shape[0]
    tile = tile_of(size)
    for start in range(0, size, tile):
        rows, cols = pl.ds(start, tile), pl.ds(0, start + tile)
        store(start, product(both[:, : start + tile], high[rows, cols], low[rows, cols], True))


def sends(odd, field, high, low, pair_ref, cross_ref):
    tile = tile_of(field.shape[1])

    def store(start, part):
        cols = pl.ds(start, tile)
        own = field[:, start : start + tile]
        pair_ref[:, cols] = jnp.where(odd, own, part)
        cross_ref[:, cols] = jnp.where(odd, part, own)

    coupling(stacked(field), high, low, store)


def begin_kernel(odd_ref, next_ref, field_ref, high_ref, low_ref, pair_ref, cross_ref, raw, sems):
    size = raw.shape[0]
    tile = tile_of(size)
    copies = []
    for index, start in enumerate(range(0, size, tile)):
        part = (pl.ds(start, tile), pl.ds(0, start + tile))
        copies.append(pltpu.make_async_copy(next_ref.at[part], raw.at[part], sems.at[index]))
        copies[-1].start()
    for index, start in enumerate(range(0, size, tile)):
        part = (pl.ds(start, tile), pl.ds(0, start + tile))
        copies[index].wait()
        high, low = halves(raw[part])
        high_ref[part] = high
        low_ref[part] = low
    sends(odd_ref[0] == 1, field_ref[...], high_ref, low_ref, pair_ref, cross_ref)


def local_kernel(local_ref, field_ref, high_ref, low_ref, own_ref):
    size = local_ref.shape[0]
    tile = tile_of(size)
    both = stacked(field_ref[...])
    total = None
    for start in range(0, size, tile):
        rows = pl.ds(start, tile)
        row = lax.broadcasted_iota(jnp.int32, (tile, size), 0) + start
        col = lax.broadcasted_iota(jnp.int32, (tile, size), 1)
        high, low = halves(local_ref[rows, :] - jnp.where(row == col, 1.0, 0.0))
        high_ref[rows, :] = high
        low_ref[rows, :] = low
        part = product(both[:, start : start + tile], high, low)
        total = part if total is None else total + part
    own_ref[...] = total


def moment(left, right):
    return jnp.sum(left * right, axis=1, keepdims=True)


def own_kernel(before_ref, field_ref, high_ref, low_ref, own_ref, moments_ref):
    field = field_ref[...]
    own_ref[...] = product(stacked(field), high_ref[...], low_ref[...])
    lane = lax.broadcasted_iota(jnp.int32, moments_ref.shape, 1)
    cross = 0.0 if before_ref is None else moment(before_ref[...], field)
    moments_ref[...] = jnp.where(lane == 0, moment(field, field), jnp.where(lane == 1, cross, 0.0))


def received(odd, pair_ref, cross_ref):
    upper = jnp.where(odd, cross_ref[...], pair_ref[...])
    lower = jnp.where(odd, pair_ref[...], cross_ref[...])
    return upper, lower


def first_kernel(
    odd_ref, own_ref, got_pair_ref, got_cross_ref, high_in, low_in, shrinkage_ref, marginal_ref, start_ref,
    field_ref, pair_ref, cross_ref,
):
    odd = odd_ref[0] == 1
    tile = tile_of(own_ref.shape[1])
    upper, lower = received(odd, got_pair_ref, got_cross_ref)
    base = marginal_ref[...] - (1.0 + shrinkage_ref[...]) * start_ref[...] - own_ref[...] - lower

    def store(start, part):
        field_ref[:, pl.ds(start, tile)] = base[:, start : start + tile] - part

    forward(stacked(upper), high_in, low_in, store)
    sends(odd, field_ref[...], high_in, low_in, pair_ref, cross_ref)


def step_kernel(
    odd_ref, own_ref, got_pair_ref, got_cross_ref, high_in, low_in, field_ref, pair_ref, cross_ref,
):
    odd = odd_ref[0] == 1
    tile = tile_of(own_ref.shape[1])
    upper, lower = received(odd, got_pair_ref, got_cross_ref)
    base = own_ref[...] + lower

    def store(start, part):
        field_ref[:, pl.ds(start, tile)] = base[:, start : start + tile] + part

    forward(stacked(upper), high_in, low_in, store)
    sends(odd, field_ref[...], high_in, low_in, pair_ref, cross_ref)


def reduce_kernel(odd_ref, field_ref, own_ref, got_pair_ref, got_cross_ref, one_ref, two_ref, three_ref, out_ref):
    odd = odd_ref[0] == 1
    _, lower = received(odd, got_pair_ref, got_cross_ref)
    traits = field_ref.shape[0]
    last = moment(field_ref[...], own_ref[...] + 2.0 * lower)
    lane = lax.broadcasted_iota(jnp.int32, (traits, 128), 1)
    parts = (
        one_ref[:, 0:1],
        two_ref[:, 1:2],
        two_ref[:, 0:1],
        three_ref[:, 1:2],
        three_ref[:, 0:1],
        last,
    )
    table = jnp.zeros((traits, 128), F32)
    for index, part in enumerate(parts):
        table = jnp.where(lane == index, part, table)
    rows = jnp.transpose(table)[:MOMENT_ROWS]
    for index in range(out_ref.shape[0]):
        out_ref[index] = rows


def coefficients(moments, shift):
    def inner(left, right):
        total = None
        for i, a in enumerate(left):
            for j, b in enumerate(right):
                term = (a * b) * moments[i + j]
                total = term if total is None else total + term
        return total

    one = jnp.ones_like(shift)
    zero = jnp.zeros_like(shift)
    residual, direction, gain = [one], [one], []
    norm_now = moments[0]
    for step in range(ITERS):
        image = [shift * a + b for a, b in zip(direction + [zero], [zero] + direction)]
        alpha = norm_now / inner(direction, image)
        gain = [a + alpha * b for a, b in zip(gain + [zero], direction)]
        residual = [a - alpha * b for a, b in zip(residual + [zero], image)]
        if step + 1 < ITERS:
            norm_next = inner(residual, residual)
            ratio = norm_next / norm_now
            direction = [a + ratio * b for a, b in zip(residual, direction + [zero])]
            norm_now = norm_next
    return gain, residual


def final_kernel(
    odd_ref, table_ref, shrinkage_ref, start_ref, zero_ref, one_ref, two_ref, own_ref, got_pair_ref, got_cross_ref,
    high_in, low_in, solution_ref, residual_ref,
):
    odd = odd_ref[0] == 1
    traits, size = own_ref.shape
    tile = tile_of(size)
    upper, lower = received(odd, got_pair_ref, got_cross_ref)
    sums = jnp.sum(table_ref[...], axis=0)
    columns = jnp.transpose(jnp.concatenate([sums, jnp.zeros((128 - MOMENT_ROWS, traits), F32)], axis=0))
    moments = [columns[:, i : i + 1] for i in range(2 * ITERS)]
    gain, residual = coefficients(moments, 1.0 + shrinkage_ref[...])
    zero, one, two = zero_ref[...], one_ref[...], two_ref[...]
    solution_ref[...] = start_ref[...] + gain[0] * zero + gain[1] * one + gain[2] * two
    base = residual[0] * zero + residual[1] * one + residual[2] * two + residual[3] * (own_ref[...] + lower)

    def store(start, part):
        residual_ref[:, pl.ds(start, tile)] = base[:, start : start + tile] + residual[3] * part

    forward(stacked(upper), high_in, low_in, store)


def call(kernel, out, *args, spaces=None, scratch=(), limit=32):
    shapes = [jax.ShapeDtypeStruct(shape, dtype) for shape, dtype in out]
    spaces = spaces or {}
    specs = [
        pl.BlockSpec(memory_space=spaces.get(i, VMEM)) for i in range(len(args))
    ]
    return pl.pallas_call(
        kernel,
        out_shape=shapes,
        in_specs=specs,
        out_specs=[pl.BlockSpec(memory_space=VMEM) for _ in shapes],
        scratch_shapes=scratch,
        compiler_params=pltpu.CompilerParams(vmem_limit_bytes=limit * 1024 * 1024),
    )(*args)


def on_device(local_block, next_block, shrinkage, marginal, warm_start):
    count = lax.axis_size("snp")
    odd = lax.rem(lax.axis_index("snp"), 2).astype(jnp.int32).reshape(1)
    traits, size = warm_start.shape
    field = ((traits, size), F32)
    matrix = ((size, size), BF16)
    steps = size // tile_of(size)
    on_chip = [(i, i ^ 1) for i in range(count) if i ^ 1 < count]
    off_chip = [(i, ((i - 1) ^ 1) + 1) for i in range(1, count) if ((i - 1) ^ 1) + 1 < count]
    smem = {0: pltpu.SMEM}

    def swap(pair, cross):
        got_cross = lax.ppermute(cross, "snp", off_chip)
        got_pair = lax.ppermute(pair, "snp", on_chip)
        return got_pair, got_cross

    high_n, low_n, pair, cross = call(
        begin_kernel,
        [matrix, matrix, field, field],
        odd, next_block, warm_start,
        spaces={0: pltpu.SMEM, 1: pl.ANY},
        scratch=(pltpu.VMEM((size, size), F32), pltpu.SemaphoreType.DMA((steps,))),
    )
    got = swap(pair, cross)
    high_l, low_l, own = call(local_kernel, [matrix, matrix, field], local_block, warm_start)
    zero, pair, cross = call(
        first_kernel,
        [field, field, field],
        odd, own, *got, high_n, low_n, shrinkage, marginal, warm_start,
        spaces=smem,
    )
    got = swap(pair, cross)
    table = ((traits, 128), F32)
    fields, tables = [zero], []
    for step in range(ITERS):
        if step == 0:
            own, part = call(
                lambda *refs: own_kernel(None, *refs), [field, table], fields[0], high_l, low_l
            )
        else:
            own, part = call(own_kernel, [field, table], fields[-2], fields[-1], high_l, low_l)
        tables.append(part)
        if step + 1 < ITERS:
            after, pair, cross = call(
                step_kernel, [field, field, field], odd, own, *got, high_n, low_n, spaces=smem
            )
            got = swap(pair, cross)
            fields.append(after)
    (moments,) = call(
        reduce_kernel,
        [((count, MOMENT_ROWS, traits), F32)],
        odd, fields[-1], own, *got, *tables,
        spaces=smem,
    )
    moments = lax.all_to_all(moments, "snp", 0, 0)
    return tuple(
        call(
            final_kernel,
            [field, field],
            odd, moments, shrinkage, warm_start, *fields, own, *got, high_n, low_n,
            spaces=smem,
        )
    )


def solution(mesh):
    return jax.shard_map(
        on_device,
        mesh=mesh,
        in_specs=(
            P(("parts", "snp"), None),
            P(("parts", "snp"), None),
            P(),
            P(None, ("parts", "snp")),
            P(None, ("parts", "snp")),
        ),
        out_specs=(P(None, ("parts", "snp")), P(None, ("parts", "snp"))),
        check_vma=False,
    )
```

```python
import jax
import jax.numpy as jnp
from jax import lax
from jax.experimental import pallas as pl
from jax.experimental.pallas import tpu as pltpu
from jax.sharding import PartitionSpec as P


ITERS = 3
F32 = jnp.float32
BF16 = jnp.bfloat16
VMEM = pltpu.VMEM
MOMENT_ROWS = 8


def tile_of(size):
    return 256 if size % 256 == 0 else size


def is_odd():
    return lax.rem(lax.axis_index("snp"), 2) == 1


def halves(x):
    high = x.astype(BF16)
    return high, (x - high.astype(F32)).astype(BF16)


def dot(left, right):
    return jnp.dot(left, right, preferred_element_type=F32)


def product(both, right_high, right_low):
    rows = both.shape[0] // 2
    main = dot(both, right_high)
    return main[:rows] + main[rows:] + dot(both[:rows], right_low)


def stacked(field):
    return jnp.concatenate(halves(field), axis=0)


def coupling(both, high, low, store):
    size = high.shape[0]
    tile = tile_of(size)
    for start in range(0, size, tile):
        rows, cols = pl.ds(start, size - start), pl.ds(start, tile)
        store(start, product(both[:, start:], high[rows, cols], low[rows, cols]))


def forward(both, high, low, store):
    size = high.shape[0]
    tile = tile_of(size)
    for start in range(0, size, tile):
        rows, cols = pl.ds(0, start + tile), pl.ds(start, tile)
        store(start, product(both[:, : start + tile], high[rows, cols], low[rows, cols]))


def sends(odd, field, high, low, pair_ref, cross_ref):
    tile = tile_of(field.shape[1])

    def store(start, part):
        cols = pl.ds(start, tile)
        own = field[:, start : start + tile]
        pair_ref[:, cols] = jnp.where(odd, own, part)
        cross_ref[:, cols] = jnp.where(odd, part, own)

    coupling(stacked(field), high, low, store)


def begin_kernel(next_ref, start_ref, high_ref, low_ref, pair_ref, cross_ref, raw, field, total, sems, field_sem):
    size = raw.shape[0]
    tile = tile_of(size)
    odd = is_odd()
    starts = list(range(0, size, tile))
    field_copy = pltpu.make_async_copy(start_ref, field, field_sem)
    field_copy.start()
    copies = []
    for index, start in enumerate(starts):
        part = (pl.ds(start, tile), pl.ds(0, start + tile))
        copies.append(pltpu.make_async_copy(next_ref.at[part], raw.at[part], sems.at[index]))
        copies[-1].start()
    field_copy.wait()
    for index, start in enumerate(starts):
        part = (pl.ds(start, tile), pl.ds(0, start + tile))
        copies[index].wait()
        high, low = halves(raw[part])
        high_ref[part] = high
        low_ref[part] = low
        done = product(stacked(field[:, pl.ds(start, tile)]), high, low)
        if start:
            done_before = total[:, pl.ds(0, start)] + done[:, :start]
            total[:, pl.ds(0, start)] = done_before
        total[:, pl.ds(start, tile)] = done[:, start:]
    own = field[...]
    pair_ref[...] = jnp.where(odd, own, total[...])
    cross_ref[...] = jnp.where(odd, total[...], own)


def flip_kernel(high_in, low_in, high_ref, low_ref):
    size = high_in.shape[0]
    tile = tile_of(size)
    for row in range(0, size, tile):
        for col in range(0, row + tile, tile):
            source, target = (pl.ds(row, tile), pl.ds(col, tile)), (pl.ds(col, tile), pl.ds(row, tile))
            high_ref[target] = jnp.transpose(high_in[source])
            low_ref[target] = jnp.transpose(low_in[source])


def local_kernel(
    local_ref, field_ref, marginal_ref, shrinkage_ref, pair_in, high_ref, low_ref, rest_ref, shift_ref, pair_ref
):
    del pair_in, pair_ref
    size = local_ref.shape[0]
    tile = tile_of(size)
    both = stacked(field_ref[...])
    total = None
    for start in range(0, size, tile):
        rows = pl.ds(start, tile)
        row = lax.broadcasted_iota(jnp.int32, (tile, size), 0) + start
        col = lax.broadcasted_iota(jnp.int32, (tile, size), 1)
        high, low = halves(local_ref[rows, :] - jnp.where(row == col, 1.0, 0.0))
        high_ref[rows, :] = high
        low_ref[rows, :] = low
        part = product(both[:, start : start + tile], high, low)
        total = part if total is None else total + part
    traits = field_ref.shape[0]
    here = lax.broadcasted_iota(jnp.int32, (traits, traits), 0) == lax.broadcasted_iota(jnp.int32, (traits, traits), 1)
    ridge = jnp.sum(jnp.where(here, shrinkage_ref[...], 0.0), axis=1, keepdims=True)
    shift = 1.0 + ridge
    shift_ref[...] = jnp.broadcast_to(shift, shift_ref.shape)
    rest_ref[...] = marginal_ref[...] - shift * field_ref[...] - total


def moment(left, right):
    return jnp.sum(left * right, axis=1, keepdims=True)


def own_kernel(before_ref, field_ref, high_ref, low_ref, pair_in, own_ref, moments_ref, pair_ref):
    del pair_in, pair_ref
    field = field_ref[...]
    own_ref[...] = product(stacked(field), high_ref[...], low_ref[...])
    lane = lax.broadcasted_iota(jnp.int32, moments_ref.shape, 1)
    cross = 0.0 if before_ref is None else moment(before_ref[...], field)
    moments_ref[...] = jnp.where(lane == 0, moment(field, field), jnp.where(lane == 1, cross, 0.0))


def received(odd, pair_ref, cross_ref):
    upper = jnp.where(odd, cross_ref[...], pair_ref[...])
    lower = jnp.where(odd, pair_ref[...], cross_ref[...])
    return upper, lower


def first_kernel(
    rest_ref, got_pair_ref, got_cross_ref, high_in, low_in, high_up, low_up, field_ref, pair_ref, cross_ref,
):
    odd = is_odd()
    tile = tile_of(rest_ref.shape[1])
    upper, lower = received(odd, got_pair_ref, got_cross_ref)
    base = rest_ref[...] - lower

    def store(start, part):
        field_ref[:, pl.ds(start, tile)] = base[:, start : start + tile] - part

    forward(stacked(upper), high_up, low_up, store)
    sends(odd, field_ref[...], high_in, low_in, pair_ref, cross_ref)


def step_kernel(
    own_ref, got_pair_ref, got_cross_ref, high_in, low_in, high_up, low_up, field_ref, pair_ref,
    cross_ref,
):
    odd = is_odd()
    tile = tile_of(own_ref.shape[1])
    upper, lower = received(odd, got_pair_ref, got_cross_ref)
    base = own_ref[...] + lower

    def store(start, part):
        field_ref[:, pl.ds(start, tile)] = base[:, start : start + tile] + part

    forward(stacked(upper), high_up, low_up, store)
    sends(odd, field_ref[...], high_in, low_in, pair_ref, cross_ref)


def reduce_kernel(field_ref, own_ref, got_pair_ref, got_cross_ref, one_ref, two_ref, three_ref, out_ref):
    odd = is_odd()
    _, lower = received(odd, got_pair_ref, got_cross_ref)
    traits = field_ref.shape[0]
    last = moment(field_ref[...], own_ref[...] + 2.0 * lower)
    lane = lax.broadcasted_iota(jnp.int32, (traits, 128), 1)
    parts = (
        one_ref[:, 0:1],
        two_ref[:, 1:2],
        two_ref[:, 0:1],
        three_ref[:, 1:2],
        three_ref[:, 0:1],
        last,
    )
    table = jnp.zeros((traits, 128), F32)
    for index, part in enumerate(parts):
        table = jnp.where(lane == index, part, table)
    lanes = out_ref.shape[2]
    if lanes > traits:
        table = jnp.concatenate([table, jnp.zeros((lanes - traits, 128), F32)], axis=0)
    rows = jnp.transpose(table)[:MOMENT_ROWS]
    for index in range(out_ref.shape[0]):
        out_ref[index] = rows


def coefficients(moments, shift):
    def inner(left, right):
        total = None
        for i, a in enumerate(left):
            for j, b in enumerate(right):
                term = (a * b) * moments[i + j]
                total = term if total is None else total + term
        return total

    one = jnp.ones_like(shift)
    zero = jnp.zeros_like(shift)
    residual, direction, gain = [one], [one], []
    norm_now = moments[0]
    for step in range(ITERS):
        image = [shift * a + b for a, b in zip(direction + [zero], [zero] + direction)]
        alpha = norm_now / inner(direction, image)
        gain = [a + alpha * b for a, b in zip(gain + [zero], direction)]
        residual = [a - alpha * b for a, b in zip(residual + [zero], image)]
        if step + 1 < ITERS:
            norm_next = inner(residual, residual)
            ratio = norm_next / norm_now
            direction = [a + ratio * b for a, b in zip(residual, direction + [zero])]
            norm_now = norm_next
    return gain, residual


def final_kernel(
    table_ref, shift_ref, start_ref, zero_ref, one_ref, two_ref, own_ref, got_pair_ref, got_cross_ref,
    high_up, low_up, solution_ref, residual_ref,
):
    odd = is_odd()
    traits, size = own_ref.shape
    tile = tile_of(size)
    upper, lower = received(odd, got_pair_ref, got_cross_ref)
    sums = jnp.sum(table_ref[...], axis=0)
    square = jnp.concatenate([sums, jnp.zeros((sums.shape[1] - MOMENT_ROWS, sums.shape[1]), F32)], axis=0)
    columns = jnp.transpose(square)[:traits]
    moments = [columns[:, i : i + 1] for i in range(2 * ITERS)]
    gain, residual = coefficients(moments, shift_ref[:, 0:1])
    zero, one, two = zero_ref[...], one_ref[...], two_ref[...]
    solution_ref[...] = start_ref[...] + gain[0] * zero + gain[1] * one + gain[2] * two
    base = residual[0] * zero + residual[1] * one + residual[2] * two + residual[3] * (own_ref[...] + lower)

    def store(start, part):
        residual_ref[:, pl.ds(start, tile)] = base[:, start : start + tile] + residual[3] * part

    forward(stacked(upper), high_up, low_up, store)


def call(kernel, out, *args, spaces=None, scratch=(), limit=12, aliases=None, keep=True, flops=0):
    spaces = spaces or {}
    places = [spaces.get(i, VMEM) for i in range(len(args))]
    args = [
        arg if place is pltpu.SMEM else pltpu.with_memory_space_constraint(arg, place)
        for arg, place in zip(args, places)
    ]
    make = VMEM if keep else jax.ShapeDtypeStruct
    return pl.pallas_call(
        kernel,
        out_shape=[make(shape, dtype) for shape, dtype in out],
        in_specs=[pl.BlockSpec(memory_space=place) for place in places],
        out_specs=[pl.BlockSpec(memory_space=VMEM) for _ in out],
        scratch_shapes=scratch,
        input_output_aliases=aliases or {},
        cost_estimate=pl.CostEstimate(flops=flops, bytes_accessed=0, transcendentals=0) if flops else None,
        compiler_params=pltpu.CompilerParams(vmem_limit_bytes=limit * 1024 * 1024),
    )(*args)


def on_device(local_block, next_block, shrinkage, marginal, warm_start):
    count = lax.axis_size("snp")
    traits, size = warm_start.shape
    field = ((traits, size), F32)
    matrix = ((size, size), BF16)
    steps = size // tile_of(size)
    work = 6 * traits * size * size
    on_chip = [(i, i ^ 1) for i in range(count) if i ^ 1 < count]
    off_chip = [(i, ((i - 1) ^ 1) + 1) for i in range(1, count) if ((i - 1) ^ 1) + 1 < count]

    def swap_off(cross):
        return lax.ppermute(cross, "snp", off_chip)

    def swap_on(pair):
        return lax.ppermute(pair, "snp", on_chip)

    high_n, low_n, pair, cross = call(
        begin_kernel,
        [matrix, matrix, field, field],
        next_block, warm_start,
        spaces={0: pltpu.HBM, 1: pltpu.HBM},
        scratch=(
            pltpu.VMEM((size, size), F32),
            pltpu.VMEM((traits, size), F32),
            pltpu.VMEM((traits, size), F32),
            pltpu.SemaphoreType.DMA((steps,)),
            pltpu.SemaphoreType.DMA,
        ),
    )
    got_cross = swap_off(cross)
    table = ((traits, 128), F32)
    high_l, low_l, rest, shift, pair = call(
        local_kernel,
        [matrix, matrix, field, table, field],
        local_block, warm_start, marginal, shrinkage.reshape(1, traits), pair,
        aliases={4: 4},
        flops=work,
    )
    got_pair = swap_on(pair)
    up = call(flip_kernel, [matrix, matrix], high_n, low_n, flops=work)
    zero, pair, cross = call(
        first_kernel,
        [field, field, field],
        rest, got_pair, got_cross, high_n, low_n, *up,
    )
    fields, tables = [zero], []
    for step in range(ITERS):
        before = fields[-2:-1]
        kernel = own_kernel if before else lambda *refs: own_kernel(None, *refs)
        got_cross = swap_off(cross)
        own, part, pair = call(
            kernel,
            [field, table, field],
            *before, fields[-1], high_l, low_l, pair,
            aliases={3 + len(before): 2},
            flops=work,
        )
        got_pair = swap_on(pair)
        tables.append(part)
        if step + 1 < ITERS:
            after, pair, cross = call(
                step_kernel,
                [field, field, field],
                own, got_pair, got_cross, high_n, low_n, *up,
            )
            fields.append(after)
    lanes = -(-traits // 128) * 128
    (moments,) = call(
        reduce_kernel,
        [((count, MOMENT_ROWS, lanes), F32)],
        fields[-1], own, got_pair, got_cross, *tables,
    )
    moments = lax.all_to_all(moments, "snp", 0, 0)
    return tuple(
        call(
            final_kernel,
            [field, field],
            moments, shift, warm_start, *fields, own, got_pair, got_cross, *up,
            keep=False,
        )
    )


def solution(mesh):
    return jax.shard_map(
        on_device,
        mesh=mesh,
        in_specs=(
            P(("parts", "snp"), None),
            P(("parts", "snp"), None),
            P(),
            P(None, ("parts", "snp")),
            P(None, ("parts", "snp")),
        ),
        out_specs=(P(None, ("parts", "snp")), P(None, ("parts", "snp"))),
        check_vma=False,
    )
```

```python
import functools

import jax
import jax.numpy as jnp
from jax import lax
from jax.experimental import pallas as pl
from jax.experimental.pallas import tpu as pltpu
from jax.sharding import PartitionSpec as P


ITERS = 3
F32 = jnp.float32
BF16 = jnp.bfloat16
VMEM = pltpu.VMEM
MOMENT_ROWS = 8


def tile_of(size):
    return 256 if size % 256 == 0 else size


def is_odd():
    return lax.rem(lax.axis_index("snp"), 2) == 1


def halves(x):
    high = x.astype(BF16)
    return high, (x - high.astype(F32)).astype(BF16)


def dot(left, right):
    return jnp.dot(left, right, preferred_element_type=F32)


def product(both, right_high, right_low):
    rows = both.shape[0] // 2
    main = dot(both, right_high)
    return main[:rows] + main[rows:] + dot(both[:rows], right_low)


def stacked(field):
    return jnp.concatenate(halves(field), axis=0)


def coupling(both, high, low, store):
    size = high.shape[0]
    tile = tile_of(size)
    for start in range(0, size, tile):
        rows, cols = pl.ds(start, size - start), pl.ds(start, tile)
        store(start, product(both[:, start:], high[rows, cols], low[rows, cols]))


def forward(both, high, low, store):
    size = high.shape[0]
    tile = tile_of(size)
    for start in range(0, size, tile):
        rows, cols = pl.ds(0, start + tile), pl.ds(start, tile)
        store(start, product(both[:, : start + tile], high[rows, cols], low[rows, cols]))


def split_next(next_ref, high_ref, low_ref, field, store, raw, sems):
    size = raw.shape[0]
    tile = tile_of(size)
    starts = list(range(0, size, tile))
    parts = [(pl.ds(start, tile), pl.ds(0, start + tile)) for start in starts]
    copies = [
        pltpu.make_async_copy(next_ref.at[part], raw.at[part], sems.at[index]) for index, part in enumerate(parts)
    ]
    for copy in copies:
        copy.start()
    for start, part, copy in zip(starts, parts, copies):
        copy.wait()
        high, low = halves(raw[part])
        high_ref[part] = high
        low_ref[part] = low
        store(start, product(stacked(field[:, pl.ds(start, tile)]), high, low))


def adding(total_ref):
    def store(start, part):
        tile = part.shape[1] - start
        if start:
            total_ref[:, pl.ds(0, start)] = total_ref[:, pl.ds(0, start)] + part[:, :start]
        total_ref[:, pl.ds(start, tile)] = part[:, start:]

    return store


def begin_odd_kernel(next_ref, field_ref, high_ref, low_ref, cross_ref, raw, sems):
    @pl.when(is_odd())
    def _():
        split_next(next_ref, high_ref, low_ref, field_ref, adding(cross_ref), raw, sems)


def begin_even_kernel(next_ref, field_ref, high_in, low_in, high_ref, low_ref, pair_ref, raw, sems):
    del high_in, low_in

    @pl.when(jnp.logical_not(is_odd()))
    def _():
        split_next(next_ref, high_ref, low_ref, field_ref, adding(pair_ref), raw, sems)

    @pl.when(is_odd())
    def _():
        pair_ref[...] = field_ref[...]


def flip_kernel(high_in, low_in, high_ref, low_ref):
    size = high_in.shape[0]
    tile = tile_of(size)
    for row in range(0, size, tile):
        for col in range(0, row + tile, tile):
            source, target = (pl.ds(row, tile), pl.ds(col, tile)), (pl.ds(col, tile), pl.ds(row, tile))
            high_ref[target] = jnp.transpose(high_in[source])
            low_ref[target] = jnp.transpose(low_in[source])


def local_kernel(local_ref, field_ref, marginal_ref, shrinkage_ref, high_ref, low_ref, rest_ref, shift_ref):
    size = local_ref.shape[0]
    tile = tile_of(size)
    both = stacked(field_ref[...])
    total = None
    for start in range(0, size, tile):
        rows = pl.ds(start, tile)
        row = lax.broadcasted_iota(jnp.int32, (tile, size), 0) + start
        col = lax.broadcasted_iota(jnp.int32, (tile, size), 1)
        high, low = halves(local_ref[rows, :] - jnp.where(row == col, 1.0, 0.0))
        high_ref[rows, :] = high
        low_ref[rows, :] = low
        part = product(both[:, start : start + tile], high, low)
        total = part if total is None else total + part
    traits = field_ref.shape[0]
    here = lax.broadcasted_iota(jnp.int32, (traits, traits), 0) == lax.broadcasted_iota(jnp.int32, (traits, traits), 1)
    ridge = jnp.sum(jnp.where(here, shrinkage_ref[...], 0.0), axis=1, keepdims=True)
    shift = 1.0 + ridge
    shift_ref[...] = jnp.broadcast_to(shift, shift_ref.shape)
    rest_ref[...] = marginal_ref[...] - shift * field_ref[...] - total


def moment(left, right):
    return jnp.sum(left * right, axis=1, keepdims=True)


def own_kernel(before_ref, field_ref, high_ref, low_ref, own_ref, moments_ref):
    field = field_ref[...]
    own_ref[...] = product(stacked(field), high_ref[...], low_ref[...])
    lane = lax.broadcasted_iota(jnp.int32, moments_ref.shape, 1)
    cross = 0.0 if before_ref is None else moment(before_ref[...], field)
    moments_ref[...] = jnp.where(lane == 0, moment(field, field), jnp.where(lane == 1, cross, 0.0))


def pair_kernel(sign, own_ref, got_pair_ref, high_up, low_up, base_ref):
    @pl.when(is_odd())
    def _():
        base_ref[...] = own_ref[...] + sign * got_pair_ref[...]

    @pl.when(jnp.logical_not(is_odd()))
    def _():
        tile = tile_of(own_ref.shape[1])

        def store(start, part):
            cols = pl.ds(start, tile)
            base_ref[:, cols] = own_ref[:, cols] + sign * part

        forward(stacked(got_pair_ref[...]), high_up, low_up, store)


def even_kernel(sign, base_ref, got_ref, after_ref, field_ref):
    del after_ref

    @pl.when(jnp.logical_not(is_odd()))
    def _():
        field_ref[...] = base_ref[...] + sign * got_ref[...]


def odd_kernel(sign, base_ref, got_ref, high_in, low_in, high_up, low_up, after_ref, field_ref, cross_ref):
    del after_ref

    @pl.when(is_odd())
    def _():
        tile = tile_of(base_ref.shape[1])

        def keep(start, part):
            cols = pl.ds(start, tile)
            field_ref[:, cols] = base_ref[:, cols] + sign * part

        def send(start, part):
            cross_ref[:, pl.ds(start, tile)] = part

        forward(stacked(got_ref[...]), high_up, low_up, keep)
        coupling(stacked(field_ref[...]), high_in, low_in, send)


def merge_kernel(even_ref, odd_ref, high_in, low_in, field_ref, pair_ref):
    @pl.when(is_odd())
    def _():
        field_ref[...] = odd_ref[...]
        pair_ref[...] = odd_ref[...]

    @pl.when(jnp.logical_not(is_odd()))
    def _():
        tile = tile_of(even_ref.shape[1])

        def send(start, part):
            pair_ref[:, pl.ds(start, tile)] = part

        field_ref[...] = even_ref[...]
        coupling(stacked(even_ref[...]), high_in, low_in, send)


def reduce_kernel(field_ref, own_ref, got_pair_ref, got_up_ref, base_ref, one_ref, two_ref, three_ref, out_ref):
    del base_ref
    traits = field_ref.shape[0]
    lower = jnp.where(is_odd(), got_pair_ref[...], got_up_ref[...])
    last = moment(field_ref[...], own_ref[...] + 2.0 * lower)
    lane = lax.broadcasted_iota(jnp.int32, (traits, 128), 1)
    parts = (
        one_ref[:, 0:1],
        two_ref[:, 1:2],
        two_ref[:, 0:1],
        three_ref[:, 1:2],
        three_ref[:, 0:1],
        last,
    )
    table = jnp.zeros((traits, 128), F32)
    for index, part in enumerate(parts):
        table = jnp.where(lane == index, part, table)
    lanes = out_ref.shape[2]
    if lanes > traits:
        table = jnp.concatenate([table, jnp.zeros((lanes - traits, 128), F32)], axis=0)
    rows = jnp.transpose(table)[:MOMENT_ROWS]
    for index in range(out_ref.shape[0]):
        out_ref[index] = rows


def coefficients(moments, shift):
    def inner(left, right):
        total = None
        for i, a in enumerate(left):
            for j, b in enumerate(right):
                term = (a * b) * moments[i + j]
                total = term if total is None else total + term
        return total

    one = jnp.ones_like(shift)
    zero = jnp.zeros_like(shift)
    residual, direction, gain = [one], [one], []
    norm_now = moments[0]
    for step in range(ITERS):
        image = [shift * a + b for a, b in zip(direction + [zero], [zero] + direction)]
        alpha = norm_now / inner(direction, image)
        gain = [a + alpha * b for a, b in zip(gain + [zero], direction)]
        residual = [a - alpha * b for a, b in zip(residual + [zero], image)]
        if step + 1 < ITERS:
            norm_next = inner(residual, residual)
            ratio = norm_next / norm_now
            direction = [a + ratio * b for a, b in zip(residual, direction + [zero])]
            norm_now = norm_next
    return gain, residual


def weights_kernel(table_ref, shift_ref, weights_ref):
    traits = shift_ref.shape[0]
    sums = jnp.sum(table_ref[...], axis=0)
    square = jnp.concatenate([sums, jnp.zeros((sums.shape[1] - MOMENT_ROWS, sums.shape[1]), F32)], axis=0)
    columns = jnp.transpose(square)[:traits]
    moments = [columns[:, i : i + 1] for i in range(2 * ITERS)]
    gain, residual = coefficients(moments, shift_ref[:, 0:1])
    lane = lax.broadcasted_iota(jnp.int32, (traits, 128), 1)
    table = jnp.zeros((traits, 128), F32)
    for index, part in enumerate(gain + residual):
        table = jnp.where(lane == index, part, table)
    weights_ref[...] = table


def final_kernel(
    weights_ref, start_ref, zero_ref, one_ref, two_ref, base_ref, got_down_ref, got_up_ref, high_up, low_up,
    solution_ref, residual_ref,
):
    tile = tile_of(base_ref.shape[1])
    weights = [weights_ref[:, i : i + 1] for i in range(2 * ITERS + 1)]
    gain, residual = weights[:ITERS], weights[ITERS:]
    zero, one, two = zero_ref[...], one_ref[...], two_ref[...]
    solution_ref[...] = start_ref[...] + gain[0] * zero + gain[1] * one + gain[2] * two
    residual_ref[...] = residual[0] * zero + residual[1] * one + residual[2] * two + residual[3] * base_ref[...]

    @pl.when(is_odd())
    def _():
        def store(start, part):
            cols = pl.ds(start, tile)
            residual_ref[:, cols] = residual_ref[:, cols] + residual[3] * part

        forward(stacked(got_down_ref[...]), high_up, low_up, store)

    @pl.when(jnp.logical_not(is_odd()))
    def _():
        residual_ref[...] = residual_ref[...] + residual[3] * got_up_ref[...]


def call(kernel, out, *args, spaces=None, scratch=(), limit=12, aliases=None, keep=True, flops=0):
    spaces = spaces or {}
    places = [spaces.get(i, VMEM) for i in range(len(args))]
    args = [
        arg if place is pltpu.SMEM else pltpu.with_memory_space_constraint(arg, place)
        for arg, place in zip(args, places)
    ]
    make = VMEM if keep else jax.ShapeDtypeStruct
    return pl.pallas_call(
        kernel,
        out_shape=[make(shape, dtype) for shape, dtype in out],
        in_specs=[pl.BlockSpec(memory_space=place) for place in places],
        out_specs=[pl.BlockSpec(memory_space=VMEM) for _ in out],
        scratch_shapes=scratch,
        input_output_aliases=aliases or {},
        cost_estimate=pl.CostEstimate(flops=flops, bytes_accessed=0, transcendentals=0) if flops else None,
        compiler_params=pltpu.CompilerParams(vmem_limit_bytes=limit * 1024 * 1024),
    )(*args)


def on_device(local_block, next_block, shrinkage, marginal, warm_start):
    count = lax.axis_size("snp")
    traits, size = warm_start.shape
    field = ((traits, size), F32)
    table = ((traits, 128), F32)
    matrix = ((size, size), BF16)
    work = 6 * traits * size * size
    copies = (
        pltpu.VMEM((size, size), F32),
        pltpu.SemaphoreType.DMA((size // tile_of(size),)),
    )
    on_chip = [(i, i ^ 1) for i in range(count) if i ^ 1 < count]
    downward = [(i + 1, i) for i in range(count - 1)]
    upward = [(i, i + 1) for i in range(count - 1)]

    def shift(value, route):
        return lax.ppermute(value, "snp", route)

    def run(kernel, out, *args, **rest):
        return call(kernel, out, *args, **rest)

    down = shift(warm_start, downward)
    high_n, low_n, cross = run(
        begin_odd_kernel, [matrix, matrix, field], next_block, warm_start,
        spaces={0: pltpu.HBM}, scratch=copies, flops=work,
    )
    up = shift(cross, upward)
    high_n, low_n, pair = run(
        begin_even_kernel, [matrix, matrix, field], next_block, warm_start, high_n, low_n,
        spaces={0: pltpu.HBM}, scratch=copies, aliases={2: 0, 3: 1}, flops=work,
    )
    got_pair = shift(pair, on_chip)
    high_l, low_l, own, ridge = run(
        local_kernel, [matrix, matrix, field, table],
        local_block, warm_start, marginal, shrinkage.reshape(1, traits), flops=work,
    )
    flipped = run(flip_kernel, [matrix, matrix], high_n, low_n, flops=work)
    sign = -1.0
    fields, tables = [], []
    for step in range(1, ITERS + 1):
        (base,) = run(functools.partial(pair_kernel, sign), [field], own, got_pair, *flipped, flops=work)
        even = functools.partial(even_kernel, sign)
        odd = functools.partial(odd_kernel, sign)
        if step % 2:
            odd_field, cross = run(odd, [field, field], base, down, high_n, low_n, *flipped, ridge, flops=work)
            next_up = shift(cross, upward)
            (even_field,) = run(even, [field], base, up, odd_field, flops=work)
            down = shift(even_field, downward)
        else:
            (even_field,) = run(even, [field], base, up, ridge, flops=work)
            next_down = shift(even_field, downward)
            odd_field, cross = run(odd, [field, field], base, down, high_n, low_n, *flipped, even_field, flops=work)
            next_up = shift(cross, upward)
            down = next_down
        up = next_up
        merged, pair = run(merge_kernel, [field, field], even_field, odd_field, high_n, low_n, flops=work)
        got_pair = shift(pair, on_chip)
        before = fields[-1:]
        kernel = own_kernel if before else functools.partial(own_kernel, None)
        own, part = run(kernel, [field, table], *before, merged, high_l, low_l, flops=work)
        fields.append(merged)
        tables.append(part)
        sign = 1.0
    (base,) = run(functools.partial(pair_kernel, sign), [field], own, got_pair, *flipped, flops=work)
    lanes = -(-traits // 128) * 128
    (moments,) = run(reduce_kernel, [((count, MOMENT_ROWS, lanes), F32)], fields[-1], own, got_pair, up, base, *tables)
    moments = lax.all_to_all(moments, "snp", 0, 0)
    (weights,) = run(weights_kernel, [table], moments, ridge)
    return tuple(
        run(
            final_kernel, [field, field],
            weights, warm_start, *fields, base, down, up, *flipped,
            keep=False,
        )
    )


def solution(mesh):
    return jax.shard_map(
        on_device,
        mesh=mesh,
        in_specs=(
            P(("parts", "snp"), None),
            P(("parts", "snp"), None),
            P(),
            P(None, ("parts", "snp")),
            P(None, ("parts", "snp")),
        ),
        out_specs=(P(None, ("parts", "snp")), P(None, ("parts", "snp"))),
        check_vma=False,
    )
```

```python
import functools

import jax
import jax.numpy as jnp
from jax import lax
from jax.experimental import pallas as pl
from jax.experimental.pallas import tpu as pltpu
from jax.sharding import PartitionSpec as P


ITERS = 3
F32 = jnp.float32
BF16 = jnp.bfloat16
VMEM = pltpu.VMEM
MOMENT_ROWS = 8


def tile_of(size):
    return 256 if size % 256 == 0 else size


def is_odd():
    return lax.rem(lax.axis_index("snp"), 2) == 1


def halves(x):
    high = x.astype(BF16)
    return high, (x - high.astype(F32)).astype(BF16)


def dot(left, right):
    return jnp.dot(left, right, preferred_element_type=F32)


def product(both, right_high, right_low):
    rows = both.shape[0] // 2
    main = dot(both, right_high)
    return main[:rows] + main[rows:] + dot(both[:rows], right_low)


def stacked(field):
    return jnp.concatenate(halves(field), axis=0)


def coupling(both, high, low, store):
    size = high.shape[0]
    tile = tile_of(size)
    for start in range(0, size, tile):
        rows, cols = pl.ds(start, size - start), pl.ds(start, tile)
        store(start, product(both[:, start:], high[rows, cols], low[rows, cols]))


def forward(both, high, low, store):
    size = high.shape[0]
    tile = tile_of(size)
    for start in range(0, size, tile):
        rows, cols = pl.ds(0, start + tile), pl.ds(start, tile)
        store(start, product(both[:, : start + tile], high[rows, cols], low[rows, cols]))


def adding(total_ref):
    def store(start, part):
        tile = part.shape[1] - start
        if start:
            total_ref[:, pl.ds(0, start)] = total_ref[:, pl.ds(0, start)] + part[:, :start]
        total_ref[:, pl.ds(start, tile)] = part[:, start:]

    return store


def load(source_ref, parts, raw, sems):
    copies = [
        pltpu.make_async_copy(source_ref.at[part], raw.at[part], sems.at[index]) for index, part in enumerate(parts)
    ]
    for copy in copies:
        copy.start()
    return copies


def take_next(next_ref, field_ref, high_ref, low_ref, out_ref, raw, field, sems):
    size = raw.shape[0]
    tile = tile_of(size)
    starts = list(range(0, size, tile))
    parts = [(pl.ds(start, tile), pl.ds(0, start + tile)) for start in starts]
    ours = pltpu.make_async_copy(field_ref, field, sems.at[len(starts)])
    ours.start()
    copies = load(next_ref, parts, raw, sems)
    store = adding(out_ref)
    ours.wait()
    for start, part, copy in zip(starts, parts, copies):
        copy.wait()
        high, low = halves(raw[part])
        high_ref[part] = high
        low_ref[part] = low
        store(start, product(stacked(field[:, pl.ds(start, tile)]), high, low))


def take_local(local_ref, field_ref, high_ref, low_ref, out_ref, raw, field, sems):
    size = raw.shape[0]
    tile = tile_of(size)
    starts = list(range(0, size, tile))
    parts = [(pl.ds(start, tile), slice(None)) for start in starts]
    ours = pltpu.make_async_copy(field_ref, field, sems.at[len(starts)])
    ours.start()
    copies = load(local_ref, parts, raw, sems)
    ours.wait()
    for start, part, copy in zip(starts, parts, copies):
        copy.wait()
        row = lax.broadcasted_iota(jnp.int32, (tile, size), 0) + start
        col = lax.broadcasted_iota(jnp.int32, (tile, size), 1)
        high, low = halves(raw[part] - jnp.where(row == col, 1.0, 0.0))
        high_ref[part] = high
        low_ref[part] = low
        done = product(stacked(field[:, pl.ds(start, tile)]), high, low)
        out_ref[...] = done if start == 0 else out_ref[...] + done


def begin_odd_kernel(
    next_ref, local_ref, start_ref, high_n, low_n, high_l, low_l, cross_ref, own_ref, raw, field, sems
):
    @pl.when(is_odd())
    def _():
        take_next(next_ref, start_ref, high_n, low_n, cross_ref, raw, field, sems)

    @pl.when(jnp.logical_not(is_odd()))
    def _():
        take_local(local_ref, start_ref, high_l, low_l, own_ref, raw, field, sems)


def begin_even_kernel(
    next_ref, local_ref, start_ref, high_n_in, low_n_in, high_l_in, low_l_in, own_in,
    high_n, low_n, high_l, low_l, own_ref, pair_ref, raw, field, sems,
):
    del high_n_in, low_n_in, high_l_in, low_l_in, own_in

    @pl.when(is_odd())
    def _():
        take_local(local_ref, start_ref, high_l, low_l, own_ref, raw, field, sems)
        pair_ref[...] = field[...]

    @pl.when(jnp.logical_not(is_odd()))
    def _():
        take_next(next_ref, start_ref, high_n, low_n, pair_ref, raw, field, sems)


def flip_kernel(high_in, low_in, high_ref, low_ref):
    size = high_in.shape[0]
    tile = tile_of(size)
    for row in range(0, size, tile):
        for col in range(0, row + tile, tile):
            source, target = (pl.ds(row, tile), pl.ds(col, tile)), (pl.ds(col, tile), pl.ds(row, tile))
            high_ref[target] = jnp.transpose(high_in[source])
            low_ref[target] = jnp.transpose(low_in[source])


def rest_kernel(own_ref, start_ref, marginal_ref, shrinkage_ref, rest_ref, shift_ref):
    traits = start_ref.shape[0]
    here = lax.broadcasted_iota(jnp.int32, (traits, traits), 0) == lax.broadcasted_iota(jnp.int32, (traits, traits), 1)
    shift = 1.0 + jnp.sum(jnp.where(here, shrinkage_ref[...], 0.0), axis=1, keepdims=True)
    shift_ref[...] = jnp.broadcast_to(shift, shift_ref.shape)
    rest_ref[...] = marginal_ref[...] - shift * start_ref[...] - own_ref[...]


def moment(left, right):
    return jnp.sum(left * right, axis=1, keepdims=True)


def own_kernel(before_ref, field_ref, high_ref, low_ref, own_ref, moments_ref):
    field = field_ref[...]
    own_ref[...] = product(stacked(field), high_ref[...], low_ref[...])
    lane = lax.broadcasted_iota(jnp.int32, moments_ref.shape, 1)
    cross = 0.0 if before_ref is None else moment(before_ref[...], field)
    moments_ref[...] = jnp.where(lane == 0, moment(field, field), jnp.where(lane == 1, cross, 0.0))


def pair_kernel(sign, own_ref, got_pair_ref, high_up, low_up, base_ref):
    @pl.when(is_odd())
    def _():
        base_ref[...] = own_ref[...] + sign * got_pair_ref[...]

    @pl.when(jnp.logical_not(is_odd()))
    def _():
        tile = tile_of(own_ref.shape[1])

        def store(start, part):
            cols = pl.ds(start, tile)
            base_ref[:, cols] = own_ref[:, cols] + sign * part

        forward(stacked(got_pair_ref[...]), high_up, low_up, store)


def even_kernel(sign, base_ref, got_ref, after_ref, field_ref):
    del after_ref

    @pl.when(jnp.logical_not(is_odd()))
    def _():
        field_ref[...] = base_ref[...] + sign * got_ref[...]


def odd_kernel(sign, base_ref, got_ref, high_in, low_in, high_up, low_up, after_ref, field_ref, cross_ref):
    del after_ref

    @pl.when(is_odd())
    def _():
        tile = tile_of(base_ref.shape[1])

        def keep(start, part):
            cols = pl.ds(start, tile)
            field_ref[:, cols] = base_ref[:, cols] + sign * part

        def send(start, part):
            cross_ref[:, pl.ds(start, tile)] = part

        forward(stacked(got_ref[...]), high_up, low_up, keep)
        coupling(stacked(field_ref[...]), high_in, low_in, send)


def merge_kernel(even_ref, odd_ref, high_in, low_in, field_ref, pair_ref):
    @pl.when(is_odd())
    def _():
        field_ref[...] = odd_ref[...]
        pair_ref[...] = odd_ref[...]

    @pl.when(jnp.logical_not(is_odd()))
    def _():
        tile = tile_of(even_ref.shape[1])

        def send(start, part):
            pair_ref[:, pl.ds(start, tile)] = part

        field_ref[...] = even_ref[...]
        coupling(stacked(even_ref[...]), high_in, low_in, send)


def reduce_kernel(field_ref, own_ref, got_pair_ref, got_up_ref, base_ref, one_ref, two_ref, three_ref, out_ref):
    del base_ref
    traits = field_ref.shape[0]
    lower = jnp.where(is_odd(), got_pair_ref[...], got_up_ref[...])
    last = moment(field_ref[...], own_ref[...] + 2.0 * lower)
    lane = lax.broadcasted_iota(jnp.int32, (traits, 128), 1)
    parts = (
        one_ref[:, 0:1],
        two_ref[:, 1:2],
        two_ref[:, 0:1],
        three_ref[:, 1:2],
        three_ref[:, 0:1],
        last,
    )
    table = jnp.zeros((traits, 128), F32)
    for index, part in enumerate(parts):
        table = jnp.where(lane == index, part, table)
    lanes = out_ref.shape[2]
    if lanes > traits:
        table = jnp.concatenate([table, jnp.zeros((lanes - traits, 128), F32)], axis=0)
    rows = jnp.transpose(table)[:MOMENT_ROWS]
    for index in range(out_ref.shape[0]):
        out_ref[index] = rows


def coefficients(moments, shift):
    def inner(left, right):
        total = None
        for i, a in enumerate(left):
            for j, b in enumerate(right):
                term = (a * b) * moments[i + j]
                total = term if total is None else total + term
        return total

    one = jnp.ones_like(shift)
    zero = jnp.zeros_like(shift)
    residual, direction, gain = [one], [one], []
    norm_now = moments[0]
    for step in range(ITERS):
        image = [shift * a + b for a, b in zip(direction + [zero], [zero] + direction)]
        alpha = norm_now / inner(direction, image)
        gain = [a + alpha * b for a, b in zip(gain + [zero], direction)]
        residual = [a - alpha * b for a, b in zip(residual + [zero], image)]
        if step + 1 < ITERS:
            norm_next = inner(residual, residual)
            ratio = norm_next / norm_now
            direction = [a + ratio * b for a, b in zip(residual, direction + [zero])]
            norm_now = norm_next
    return gain, residual


def weights_kernel(table_ref, shift_ref, weights_ref):
    traits = shift_ref.shape[0]
    sums = jnp.sum(table_ref[...], axis=0)
    square = jnp.concatenate([sums, jnp.zeros((sums.shape[1] - MOMENT_ROWS, sums.shape[1]), F32)], axis=0)
    columns = jnp.transpose(square)[:traits]
    moments = [columns[:, i : i + 1] for i in range(2 * ITERS)]
    gain, residual = coefficients(moments, shift_ref[:, 0:1])
    lane = lax.broadcasted_iota(jnp.int32, (traits, 128), 1)
    table = jnp.zeros((traits, 128), F32)
    for index, part in enumerate(gain + residual):
        table = jnp.where(lane == index, part, table)
    weights_ref[...] = table


def final_kernel(
    weights_ref, start_ref, zero_ref, one_ref, two_ref, base_ref, got_down_ref, got_up_ref, high_up, low_up,
    solution_ref, residual_ref,
):
    tile = tile_of(base_ref.shape[1])
    weights = [weights_ref[:, i : i + 1] for i in range(2 * ITERS + 1)]
    gain, residual = weights[:ITERS], weights[ITERS:]
    zero, one, two = zero_ref[...], one_ref[...], two_ref[...]
    solution_ref[...] = start_ref[...] + gain[0] * zero + gain[1] * one + gain[2] * two
    residual_ref[...] = residual[0] * zero + residual[1] * one + residual[2] * two + residual[3] * base_ref[...]

    @pl.when(is_odd())
    def _():
        def store(start, part):
            cols = pl.ds(start, tile)
            residual_ref[:, cols] = residual_ref[:, cols] + residual[3] * part

        forward(stacked(got_down_ref[...]), high_up, low_up, store)

    @pl.when(jnp.logical_not(is_odd()))
    def _():
        residual_ref[...] = residual_ref[...] + residual[3] * got_up_ref[...]


def call(kernel, out, *args, spaces=None, scratch=(), limit=12, aliases=None, keep=True, flops=0):
    spaces = spaces or {}
    places = [spaces.get(i, VMEM) for i in range(len(args))]
    args = [
        arg if place is pltpu.SMEM else pltpu.with_memory_space_constraint(arg, place)
        for arg, place in zip(args, places)
    ]
    make = VMEM if keep else jax.ShapeDtypeStruct
    return pl.pallas_call(
        kernel,
        out_shape=[make(shape, dtype) for shape, dtype in out],
        in_specs=[pl.BlockSpec(memory_space=place) for place in places],
        out_specs=[pl.BlockSpec(memory_space=VMEM) for _ in out],
        scratch_shapes=scratch,
        input_output_aliases=aliases or {},
        cost_estimate=pl.CostEstimate(flops=flops, bytes_accessed=0, transcendentals=0) if flops else None,
        compiler_params=pltpu.CompilerParams(vmem_limit_bytes=limit * 1024 * 1024),
    )(*args)


def on_device(local_block, next_block, shrinkage, marginal, warm_start):
    count = lax.axis_size("snp")
    traits, size = warm_start.shape
    field = ((traits, size), F32)
    table = ((traits, 128), F32)
    matrix = ((size, size), BF16)
    work = 6 * traits * size * size
    copies = (
        pltpu.VMEM((size, size), F32),
        pltpu.VMEM((traits, size), F32),
        pltpu.SemaphoreType.DMA((size // tile_of(size) + 1,)),
    )
    on_chip = [(i, i ^ 1) for i in range(count) if i ^ 1 < count]
    downward = [(i + 1, i) for i in range(1, count - 1, 2)]
    upward = [(i, i + 1) for i in range(1, count - 1, 2)]

    def shift(value, route):
        return lax.ppermute(value, "snp", route)

    def run(kernel, out, *args, **rest):
        return call(kernel, out, *args, **rest)

    down = shift(warm_start, downward)
    places = {0: pltpu.HBM, 1: pltpu.HBM, 2: pltpu.HBM}
    high_n, low_n, high_l, low_l, cross, own = run(
        begin_odd_kernel, [matrix, matrix, matrix, matrix, field, field], next_block, local_block, warm_start,
        spaces=places, scratch=copies, flops=work,
    )
    up = shift(cross, upward)
    high_n, low_n, high_l, low_l, own, pair = run(
        begin_even_kernel, [matrix, matrix, matrix, matrix, field, field],
        next_block, local_block, warm_start, high_n, low_n, high_l, low_l, own,
        spaces=places, scratch=copies, aliases={3: 0, 4: 1, 5: 2, 6: 3, 7: 4}, flops=work,
    )
    got_pair = shift(pair, on_chip)
    own, ridge = run(rest_kernel, [field, table], own, warm_start, marginal, shrinkage.reshape(1, traits), flops=work)
    flipped = run(flip_kernel, [matrix, matrix], high_n, low_n, flops=work)
    sign = -1.0
    fields, tables = [], []
    for step in range(1, ITERS + 1):
        (base,) = run(functools.partial(pair_kernel, sign), [field], own, got_pair, *flipped, flops=work)
        even = functools.partial(even_kernel, sign)
        odd = functools.partial(odd_kernel, sign)
        if step % 2:
            odd_field, cross = run(odd, [field, field], base, down, high_n, low_n, *flipped, ridge, flops=work)
            next_up = shift(cross, upward)
            (even_field,) = run(even, [field], base, up, odd_field, flops=work)
            down = shift(even_field, downward)
        else:
            (even_field,) = run(even, [field], base, up, ridge, flops=work)
            next_down = shift(even_field, downward)
            odd_field, cross = run(odd, [field, field], base, down, high_n, low_n, *flipped, even_field, flops=work)
            next_up = shift(cross, upward)
            down = next_down
        up = next_up
        merged, pair = run(merge_kernel, [field, field], even_field, odd_field, high_n, low_n, flops=work)
        got_pair = shift(pair, on_chip)
        before = fields[-1:]
        kernel = own_kernel if before else functools.partial(own_kernel, None)
        own, part = run(kernel, [field, table], *before, merged, high_l, low_l, flops=work)
        fields.append(merged)
        tables.append(part)
        sign = 1.0
    (base,) = run(functools.partial(pair_kernel, sign), [field], own, got_pair, *flipped, flops=work)
    lanes = -(-traits // 128) * 128
    (moments,) = run(reduce_kernel, [((count, MOMENT_ROWS, lanes), F32)], fields[-1], own, got_pair, up, base, *tables)
    moments = lax.all_to_all(moments, "snp", 0, 0)
    (weights,) = run(weights_kernel, [table], moments, ridge)
    return tuple(
        run(
            final_kernel, [field, field],
            weights, warm_start, *fields, base, down, up, *flipped,
            keep=False,
        )
    )


def solution(mesh):
    return jax.shard_map(
        on_device,
        mesh=mesh,
        in_specs=(
            P(("parts", "snp"), None),
            P(("parts", "snp"), None),
            P(),
            P(None, ("parts", "snp")),
            P(None, ("parts", "snp")),
        ),
        out_specs=(P(None, ("parts", "snp")), P(None, ("parts", "snp"))),
        check_vma=False,
    )
```

```python
import functools

import jax
import jax.numpy as jnp
from jax import lax
from jax.experimental import pallas as pl
from jax.experimental.pallas import tpu as pltpu
from jax.sharding import PartitionSpec as P


ITERS = 3
F32 = jnp.float32
BF16 = jnp.bfloat16
VMEM = pltpu.VMEM
MOMENT_ROWS = 8


def tile_of(size):
    return 256 if size % 256 == 0 else size


def is_odd():
    return lax.rem(lax.axis_index("snp"), 2) == 1


def halves(x):
    high = x.astype(BF16)
    return high, (x - high.astype(F32)).astype(BF16)


def dot(left, right):
    return jnp.dot(left, right, preferred_element_type=F32)


def product(both, right_high, right_low):
    rows = both.shape[0] // 2
    main = dot(both, right_high)
    return main[:rows] + main[rows:] + dot(both[:rows], right_low)


def stacked(field):
    return jnp.concatenate(halves(field), axis=0)


def coupling(both, high, low, store):
    size = high.shape[0]
    tile = tile_of(size)
    for start in range(0, size, tile):
        rows, cols = pl.ds(start, size - start), pl.ds(start, tile)
        store(start, product(both[:, start:], high[rows, cols], low[rows, cols]))


def forward(both, high, low, store):
    size = high.shape[0]
    tile = tile_of(size)
    for start in range(0, size, tile):
        rows, cols = pl.ds(0, start + tile), pl.ds(start, tile)
        store(start, product(both[:, : start + tile], high[rows, cols], low[rows, cols]))


def adding(total_ref):
    def store(start, part):
        tile = part.shape[1] - start
        if start:
            total_ref[:, pl.ds(0, start)] = total_ref[:, pl.ds(0, start)] + part[:, :start]
        total_ref[:, pl.ds(start, tile)] = part[:, start:]

    return store


def load(source_ref, parts, raw, sems):
    copies = [
        pltpu.make_async_copy(source_ref.at[part], raw.at[part], sems.at[index]) for index, part in enumerate(parts)
    ]
    for copy in copies:
        copy.start()
    return copies


def take_next(next_ref, field_ref, high_ref, low_ref, out_ref, raw, field, sems):
    size = raw.shape[0]
    tile = tile_of(size)
    starts = list(range(0, size, tile))
    parts = [(pl.ds(start, tile), pl.ds(0, start + tile)) for start in starts]
    ours = pltpu.make_async_copy(field_ref, field, sems.at[len(starts)])
    ours.start()
    copies = load(next_ref, parts, raw, sems)
    store = adding(out_ref)
    ours.wait()
    for start, part, copy in zip(starts, parts, copies):
        copy.wait()
        high, low = halves(raw[part])
        high_ref[part] = high
        low_ref[part] = low
        store(start, product(stacked(field[:, pl.ds(start, tile)]), high, low))


def take_local(local_ref, field_ref, high_ref, low_ref, out_ref, raw, field, sems):
    size = raw.shape[0]
    tile = tile_of(size)
    starts = list(range(0, size, tile))
    parts = [(pl.ds(start, tile), slice(None)) for start in starts]
    ours = pltpu.make_async_copy(field_ref, field, sems.at[len(starts)])
    ours.start()
    copies = load(local_ref, parts, raw, sems)
    ours.wait()
    for start, part, copy in zip(starts, parts, copies):
        copy.wait()
        row = lax.broadcasted_iota(jnp.int32, (tile, size), 0) + start
        col = lax.broadcasted_iota(jnp.int32, (tile, size), 1)
        high, low = halves(raw[part] - jnp.where(row == col, 1.0, 0.0))
        high_ref[part] = high
        low_ref[part] = low
        done = product(stacked(field[:, pl.ds(start, tile)]), high, low)
        out_ref[...] = done if start == 0 else out_ref[...] + done


def begin_odd_kernel(next_ref, start_ref, high_n, low_n, cross_ref, raw, field, sems):
    @pl.when(is_odd())
    def _():
        take_next(next_ref, start_ref, high_n, low_n, cross_ref, raw, field, sems)


def begin_even_kernel(
    next_ref, local_ref, start_ref, high_n_in, low_n_in,
    high_n, low_n, high_l, low_l, own_ref, pair_ref, raw, field, sems,
):
    del high_n_in, low_n_in

    @pl.when(is_odd())
    def _():
        take_local(local_ref, start_ref, high_l, low_l, own_ref, raw, field, sems)
        pair_ref[...] = field[...]

    @pl.when(jnp.logical_not(is_odd()))
    def _():
        take_next(next_ref, start_ref, high_n, low_n, pair_ref, raw, field, sems)


def flip(high_in, low_in, high_ref, low_ref):
    size = high_in.shape[0]
    tile = tile_of(size)
    for row in range(0, size, tile):
        for col in range(0, row + tile, tile):
            source, target = (pl.ds(row, tile), pl.ds(col, tile)), (pl.ds(col, tile), pl.ds(row, tile))
            high_ref[target] = jnp.transpose(high_in[source])
            low_ref[target] = jnp.transpose(low_in[source])


def ridge_column(shrinkage_ref):
    traits = shrinkage_ref.shape[1]
    here = lax.broadcasted_iota(jnp.int32, (traits, traits), 0) == lax.broadcasted_iota(jnp.int32, (traits, traits), 1)
    return 1.0 + jnp.sum(jnp.where(here, shrinkage_ref[...], 0.0), axis=1, keepdims=True)


def prepare_odd_kernel(own_ref, start_ref, marginal_ref, shrinkage_ref, high_n, low_n, rest_ref, high_up, low_up):
    @pl.when(is_odd())
    def _():
        rest_ref[...] = marginal_ref[...] - ridge_column(shrinkage_ref) * start_ref[...] - own_ref[...]
        flip(high_n, low_n, high_up, low_up)


def prepare_even_kernel(
    local_ref, start_ref, marginal_ref, shrinkage_ref, got_pair_ref, high_n, low_n,
    high_l_in, low_l_in, high_up_in, low_up_in, after_ref,
    high_l, low_l, high_up, low_up, base_ref, raw, field, sems,
):
    del high_l_in, low_l_in, high_up_in, low_up_in, after_ref

    @pl.when(jnp.logical_not(is_odd()))
    def _():
        flip(high_n, low_n, high_up, low_up)
        take_local(local_ref, start_ref, high_l, low_l, base_ref, raw, field, sems)
        base_ref[...] = marginal_ref[...] - ridge_column(shrinkage_ref) * field[...] - base_ref[...]
        tile = tile_of(base_ref.shape[1])

        def store(start, part):
            cols = pl.ds(start, tile)
            base_ref[:, cols] = base_ref[:, cols] - part

        forward(stacked(got_pair_ref[...]), high_up, low_up, store)


def moment(left, right):
    return jnp.sum(left * right, axis=1, keepdims=True)


def own_kernel(before_ref, field_ref, high_ref, low_ref, own_ref, moments_ref):
    field = field_ref[...]
    own_ref[...] = product(stacked(field), high_ref[...], low_ref[...])
    lane = lax.broadcasted_iota(jnp.int32, moments_ref.shape, 1)
    cross = 0.0 if before_ref is None else moment(before_ref[...], field)
    moments_ref[...] = jnp.where(lane == 0, moment(field, field), jnp.where(lane == 1, cross, 0.0))


def pair_kernel(own_ref, got_pair_ref, high_up, low_up, base_ref):
    @pl.when(jnp.logical_not(is_odd()))
    def _():
        tile = tile_of(own_ref.shape[1])

        def store(start, part):
            cols = pl.ds(start, tile)
            base_ref[:, cols] = own_ref[:, cols] + part

        forward(stacked(got_pair_ref[...]), high_up, low_up, store)


def even_kernel(base_ref, got_ref, after_ref, field_ref):
    del after_ref

    @pl.when(jnp.logical_not(is_odd()))
    def _():
        field_ref[...] = base_ref[...] + got_ref[...]


def odd_kernel(sign, own_ref, got_pair_ref, got_ref, high_in, low_in, high_up, low_up, after_ref, field_ref, cross_ref):
    del after_ref

    @pl.when(is_odd())
    def _():
        tile = tile_of(own_ref.shape[1])

        def keep(start, part):
            cols = pl.ds(start, tile)
            field_ref[:, cols] = own_ref[:, cols] + sign * (got_pair_ref[:, cols] + part)

        def send(start, part):
            cross_ref[:, pl.ds(start, tile)] = part

        forward(stacked(got_ref[...]), high_up, low_up, keep)
        coupling(stacked(field_ref[...]), high_in, low_in, send)


def couple_even(field_ref, high_in, low_in, pair_ref):
    tile = tile_of(field_ref.shape[1])

    def send(start, part):
        pair_ref[:, pl.ds(start, tile)] = part

    coupling(stacked(field_ref[...]), high_in, low_in, send)


def merge_kernel(even_ref, odd_ref, high_in, low_in, field_ref, pair_ref):
    @pl.when(is_odd())
    def _():
        field_ref[...] = odd_ref[...]
        pair_ref[...] = odd_ref[...]

    @pl.when(jnp.logical_not(is_odd()))
    def _():
        field_ref[...] = even_ref[...]
        couple_even(field_ref, high_in, low_in, pair_ref)


def join_kernel(sign, base_ref, got_ref, odd_ref, high_in, low_in, field_ref, pair_ref):
    @pl.when(is_odd())
    def _():
        field_ref[...] = odd_ref[...]
        pair_ref[...] = odd_ref[...]

    @pl.when(jnp.logical_not(is_odd()))
    def _():
        field_ref[...] = base_ref[...] + sign * got_ref[...]
        couple_even(field_ref, high_in, low_in, pair_ref)


def reduce_kernel(field_ref, own_ref, got_pair_ref, got_up_ref, one_ref, two_ref, three_ref, out_ref):
    traits = field_ref.shape[0]
    lower = jnp.where(is_odd(), got_pair_ref[...], got_up_ref[...])
    last = moment(field_ref[...], own_ref[...] + 2.0 * lower)
    lane = lax.broadcasted_iota(jnp.int32, (traits, 128), 1)
    parts = (
        one_ref[:, 0:1],
        two_ref[:, 1:2],
        two_ref[:, 0:1],
        three_ref[:, 1:2],
        three_ref[:, 0:1],
        last,
    )
    table = jnp.zeros((traits, 128), F32)
    for index, part in enumerate(parts):
        table = jnp.where(lane == index, part, table)
    lanes = out_ref.shape[2]
    if lanes > traits:
        table = jnp.concatenate([table, jnp.zeros((lanes - traits, 128), F32)], axis=0)
    rows = jnp.transpose(table)[:MOMENT_ROWS]
    for index in range(out_ref.shape[0]):
        out_ref[index] = rows


def coefficients(moments, shift):
    def inner(left, right):
        total = None
        for i, a in enumerate(left):
            for j, b in enumerate(right):
                term = (a * b) * moments[i + j]
                total = term if total is None else total + term
        return total

    one = jnp.ones_like(shift)
    zero = jnp.zeros_like(shift)
    residual, direction, gain = [one], [one], []
    norm_now = moments[0]
    for step in range(ITERS):
        image = [shift * a + b for a, b in zip(direction + [zero], [zero] + direction)]
        alpha = norm_now / inner(direction, image)
        gain = [a + alpha * b for a, b in zip(gain + [zero], direction)]
        residual = [a - alpha * b for a, b in zip(residual + [zero], image)]
        if step + 1 < ITERS:
            norm_next = inner(residual, residual)
            ratio = norm_next / norm_now
            direction = [a + ratio * b for a, b in zip(residual, direction + [zero])]
            norm_now = norm_next
    return gain, residual


def weights_kernel(table_ref, shrinkage_ref, weights_ref):
    sums = jnp.sum(table_ref[...], axis=0)
    traits, lanes = weights_ref.shape[0], sums.shape[1]
    shift = 1.0 + shrinkage_ref[...]
    moments = [sums[i : i + 1, :traits] for i in range(2 * ITERS)]
    gain, residual = coefficients(moments, shift)
    row = lax.broadcasted_iota(jnp.int32, (lanes, traits), 0)
    table = jnp.zeros((lanes, traits), F32)
    for index, part in enumerate(gain + residual):
        table = jnp.where(row == index, part, table)
    weights_ref[...] = jnp.transpose(table)


def final_kernel(
    weights_ref, start_ref, zero_ref, one_ref, two_ref, own_ref, got_pair_ref, got_down_ref, got_up_ref,
    high_up, low_up, solution_ref, residual_ref,
):
    tile = tile_of(own_ref.shape[1])
    weights = [weights_ref[:, i : i + 1] for i in range(2 * ITERS + 1)]
    gain, residual = weights[:ITERS], weights[ITERS:]
    odd = is_odd()
    upper = jnp.where(odd, got_down_ref[...], got_pair_ref[...])
    lower = jnp.where(odd, got_pair_ref[...], got_up_ref[...])
    zero, one, two = zero_ref[...], one_ref[...], two_ref[...]
    solution_ref[...] = start_ref[...] + gain[0] * zero + gain[1] * one + gain[2] * two
    base = residual[0] * zero + residual[1] * one + residual[2] * two + residual[3] * (own_ref[...] + lower)

    def store(start, part):
        residual_ref[:, pl.ds(start, tile)] = base[:, start : start + tile] + residual[3] * part

    forward(stacked(upper), high_up, low_up, store)


def call(kernel, out, *args, spaces=None, scratch=(), limit=12, aliases=None, keep=True, flops=0):
    spaces = spaces or {}
    places = [spaces.get(i, VMEM) for i in range(len(args))]
    args = [
        arg if place is pltpu.SMEM else pltpu.with_memory_space_constraint(arg, place)
        for arg, place in zip(args, places)
    ]
    make = VMEM if keep else jax.ShapeDtypeStruct
    return pl.pallas_call(
        kernel,
        out_shape=[make(shape, dtype) for shape, dtype in out],
        in_specs=[pl.BlockSpec(memory_space=place) for place in places],
        out_specs=[pl.BlockSpec(memory_space=VMEM) for _ in out],
        scratch_shapes=scratch,
        input_output_aliases=aliases or {},
        cost_estimate=pl.CostEstimate(flops=flops, bytes_accessed=0, transcendentals=0) if flops else None,
        compiler_params=pltpu.CompilerParams(vmem_limit_bytes=limit * 1024 * 1024),
    )(*args)


def on_device(local_block, next_block, shrinkage, marginal, warm_start):
    count = lax.axis_size("snp")
    traits, size = warm_start.shape
    field = ((traits, size), F32)
    table = ((traits, 128), F32)
    matrix = ((size, size), BF16)
    work = 6 * traits * size * size
    copies = (
        pltpu.VMEM((size, size), F32),
        pltpu.VMEM((traits, size), F32),
        pltpu.SemaphoreType.DMA((size // tile_of(size) + 1,)),
    )
    on_chip = [(i, i ^ 1) for i in range(count) if i ^ 1 < count]
    downward = [(i + 1, i) for i in range(1, count - 1, 2)]
    upward = [(i, i + 1) for i in range(1, count - 1, 2)]

    def shift(value, route):
        return lax.ppermute(value, "snp", route)

    def run(kernel, out, *args, **rest):
        return call(kernel, out, *args, **rest)

    hbm = pltpu.HBM
    ridge = shrinkage.reshape(1, traits)
    down = shift(warm_start, downward)
    high_n, low_n, cross = run(
        begin_odd_kernel, [matrix, matrix, field], next_block, warm_start,
        spaces={0: hbm, 1: hbm}, scratch=copies, flops=work,
    )
    up = shift(cross, upward)
    high_n, low_n, high_l, low_l, own, pair = run(
        begin_even_kernel, [matrix, matrix, matrix, matrix, field, field],
        next_block, local_block, warm_start, high_n, low_n,
        spaces={0: hbm, 1: hbm, 2: hbm}, scratch=copies, aliases={3: 0, 4: 1}, flops=work,
    )
    got_pair = shift(pair, on_chip)
    rest, high_up, low_up = run(
        prepare_odd_kernel, [field, matrix, matrix],
        own, warm_start, marginal, ridge, high_n, low_n, flops=work,
    )
    odd = functools.partial(odd_kernel, -1.0)
    odd_field, cross = run(odd, [field, field], rest, got_pair, down, high_n, low_n, high_up, low_up, ridge, flops=work)
    next_up = shift(cross, upward)
    high_l, low_l, high_up, low_up, base = run(
        prepare_even_kernel, [matrix, matrix, matrix, matrix, field],
        local_block, warm_start, marginal, ridge, got_pair, high_n, low_n,
        high_l, low_l, high_up, low_up, odd_field,
        spaces={0: hbm, 1: hbm}, scratch=copies, aliases={7: 0, 8: 1, 9: 2, 10: 3}, flops=work,
    )
    join = functools.partial(join_kernel, -1.0)
    merged, pair = run(join, [field, field], base, up, odd_field, high_n, low_n, flops=work)
    up = next_up
    fields, tables = [merged], []
    odd, join = functools.partial(odd_kernel, 1.0), functools.partial(join_kernel, 1.0)
    for step in range(2, ITERS + 2):
        got_pair = shift(pair, on_chip)
        if step % 2 == 0:
            down = shift(merged, downward)
        before = fields[-2:-1]
        kernel = own_kernel if before else functools.partial(own_kernel, None)
        own, part = run(kernel, [field, table], *before, merged, high_l, low_l, flops=work)
        tables.append(part)
        if step > ITERS:
            break
        (base,) = run(pair_kernel, [field], own, got_pair, high_up, low_up, flops=work)
        if step % 2 == 0:
            (even_field,) = run(even_kernel, [field], base, up, ridge, flops=work)
            next_down = shift(even_field, downward)
            odd_field, cross = run(
                odd, [field, field],
                own, got_pair, down, high_n, low_n, high_up, low_up, even_field, flops=work,
            )
            up = shift(cross, upward)
            down = next_down
            merged, pair = run(merge_kernel, [field, field], even_field, odd_field, high_n, low_n, flops=work)
        else:
            odd_field, cross = run(
                odd, [field, field],
                own, got_pair, down, high_n, low_n, high_up, low_up, base, flops=work,
            )
            next_up = shift(cross, upward)
            merged, pair = run(join, [field, field], base, up, odd_field, high_n, low_n, flops=work)
            up = next_up
        fields.append(merged)
    lanes = -(-traits // 128) * 128
    (moments,) = run(reduce_kernel, [((count, MOMENT_ROWS, lanes), F32)], fields[-1], own, got_pair, up, *tables)
    moments = lax.all_to_all(moments, "snp", 0, 0)
    (weights,) = run(weights_kernel, [table], moments, ridge)
    return tuple(
        run(
            final_kernel, [field, field],
            weights, warm_start, *fields, own, got_pair, down, up, high_up, low_up,
            keep=False,
        )
    )


def solution(mesh):
    return jax.shard_map(
        on_device,
        mesh=mesh,
        in_specs=(
            P(("parts", "snp"), None),
            P(("parts", "snp"), None),
            P(),
            P(None, ("parts", "snp")),
            P(None, ("parts", "snp")),
        ),
        out_specs=(P(None, ("parts", "snp")), P(None, ("parts", "snp"))),
        check_vma=False,
    )
```

```python
import functools

import jax
import jax.numpy as jnp
from jax import lax
from jax.experimental import pallas as pl
from jax.experimental.pallas import tpu as pltpu
from jax.sharding import PartitionSpec as P


ITERS = 3
F32 = jnp.float32
BF16 = jnp.bfloat16
VMEM = pltpu.VMEM
MOMENT_ROWS = 8


def tile_of(size):
    return 256 if size % 256 == 0 else size


def is_odd():
    return lax.rem(lax.axis_index("snp"), 2) == 1


def halves(x):
    high = x.astype(BF16)
    return high, (x - high.astype(F32)).astype(BF16)


def dot(left, right):
    return jnp.dot(left, right, preferred_element_type=F32)


def product(both, right_high, right_low):
    rows = both.shape[0] // 2
    main = dot(both, right_high)
    return main[:rows] + main[rows:] + dot(both[:rows], right_low)


def stacked(field):
    return jnp.concatenate(halves(field), axis=0)


def coupling(both, high, low, store):
    size = high.shape[0]
    tile = tile_of(size)
    for start in range(0, size, tile):
        rows, cols = pl.ds(start, size - start), pl.ds(start, tile)
        store(start, product(both[:, start:], high[rows, cols], low[rows, cols]))


def forward(both, high, low, store):
    size = high.shape[0]
    tile = tile_of(size)
    for start in range(0, size, tile):
        rows, cols = pl.ds(0, start + tile), pl.ds(start, tile)
        store(start, product(both[:, : start + tile], high[rows, cols], low[rows, cols]))


def adding(total_ref):
    def store(start, part):
        tile = part.shape[1] - start
        if start:
            total_ref[:, pl.ds(0, start)] = total_ref[:, pl.ds(0, start)] + part[:, :start]
        total_ref[:, pl.ds(start, tile)] = part[:, start:]

    return store


def load(source_ref, parts, raw, sems):
    copies = [
        pltpu.make_async_copy(source_ref.at[part], raw.at[part], sems.at[index]) for index, part in enumerate(parts)
    ]
    for copy in copies:
        copy.start()
    return copies


def take_next(next_ref, field_ref, high_ref, low_ref, out_ref, raw, sems, field=None):
    size = raw.shape[0]
    tile = tile_of(size)
    starts = list(range(0, size, tile))
    parts = [(pl.ds(start, tile), pl.ds(0, start + tile)) for start in starts]
    if field is not None:
        ours = pltpu.make_async_copy(field_ref, field, sems.at[len(starts)])
        ours.start()
    copies = load(next_ref, parts, raw, sems)
    store = adding(out_ref)
    if field is not None:
        ours.wait()
        field_ref = field
    for start, part, copy in zip(starts, parts, copies):
        copy.wait()
        high, low = halves(raw[part])
        high_ref[part] = high
        low_ref[part] = low
        store(start, product(stacked(field_ref[:, pl.ds(start, tile)]), high, low))


def take_local(local_ref, field_ref, high_ref, low_ref, out_ref):
    size = local_ref.shape[0]
    tile = tile_of(size)
    both = stacked(field_ref[...])
    for start in range(0, size, tile):
        rows = pl.ds(start, tile)
        row = lax.broadcasted_iota(jnp.int32, (tile, size), 0) + start
        col = lax.broadcasted_iota(jnp.int32, (tile, size), 1)
        high, low = halves(local_ref[rows, :] - jnp.where(row == col, 1.0, 0.0))
        high_ref[rows, :] = high
        low_ref[rows, :] = low
        done = product(both[:, start : start + tile], high, low)
        out_ref[...] = done if start == 0 else out_ref[...] + done


def begin_odd_kernel(next_ref, start_ref, high_n, low_n, cross_ref, raw, field, sems):
    @pl.when(is_odd())
    def _():
        take_next(next_ref, start_ref, high_n, low_n, cross_ref, raw, sems, field)


def begin_even_kernel(
    next_ref, local_ref, start_ref, high_n_in, low_n_in,
    high_n, low_n, high_l, low_l, own_ref, pair_ref, raw, sems,
):
    del high_n_in, low_n_in

    @pl.when(is_odd())
    def _():
        take_local(local_ref, start_ref, high_l, low_l, own_ref)
        pair_ref[...] = start_ref[...]

    @pl.when(jnp.logical_not(is_odd()))
    def _():
        take_next(next_ref, start_ref, high_n, low_n, pair_ref, raw, sems)


def flip(high_in, low_in, high_ref, low_ref):
    size = high_in.shape[0]
    tile = tile_of(size)
    for row in range(0, size, tile):
        for col in range(0, row + tile, tile):
            source, target = (pl.ds(row, tile), pl.ds(col, tile)), (pl.ds(col, tile), pl.ds(row, tile))
            high_ref[target] = jnp.transpose(high_in[source])
            low_ref[target] = jnp.transpose(low_in[source])


def ridge_column(shrinkage_ref):
    traits = shrinkage_ref.shape[1]
    here = lax.broadcasted_iota(jnp.int32, (traits, traits), 0) == lax.broadcasted_iota(jnp.int32, (traits, traits), 1)
    return 1.0 + jnp.sum(jnp.where(here, shrinkage_ref[...], 0.0), axis=1, keepdims=True)


def prepare_odd_kernel(own_ref, start_ref, marginal_ref, shrinkage_ref, high_n, low_n, rest_ref, high_up, low_up):
    @pl.when(is_odd())
    def _():
        rest_ref[...] = marginal_ref[...] - ridge_column(shrinkage_ref) * start_ref[...] - own_ref[...]
        flip(high_n, low_n, high_up, low_up)


def prepare_even_kernel(
    local_ref, start_ref, marginal_ref, shrinkage_ref, got_pair_ref, high_n, low_n,
    high_l_in, low_l_in, high_up_in, low_up_in, after_ref,
    high_l, low_l, high_up, low_up, base_ref,
):
    del high_l_in, low_l_in, high_up_in, low_up_in, after_ref

    @pl.when(jnp.logical_not(is_odd()))
    def _():
        flip(high_n, low_n, high_up, low_up)
        take_local(local_ref, start_ref, high_l, low_l, base_ref)
        base_ref[...] = marginal_ref[...] - ridge_column(shrinkage_ref) * start_ref[...] - base_ref[...]
        tile = tile_of(base_ref.shape[1])

        def store(start, part):
            cols = pl.ds(start, tile)
            base_ref[:, cols] = base_ref[:, cols] - part

        forward(stacked(got_pair_ref[...]), high_up, low_up, store)


def moment(left, right):
    return jnp.sum(left * right, axis=1, keepdims=True)


def own_kernel(before_ref, field_ref, high_ref, low_ref, own_ref, moments_ref):
    field = field_ref[...]
    own_ref[...] = product(stacked(field), high_ref[...], low_ref[...])
    lane = lax.broadcasted_iota(jnp.int32, moments_ref.shape, 1)
    cross = 0.0 if before_ref is None else moment(before_ref[...], field)
    moments_ref[...] = jnp.where(lane == 0, moment(field, field), jnp.where(lane == 1, cross, 0.0))


def pair_kernel(own_ref, got_pair_ref, high_up, low_up, base_ref):
    @pl.when(jnp.logical_not(is_odd()))
    def _():
        tile = tile_of(own_ref.shape[1])

        def store(start, part):
            cols = pl.ds(start, tile)
            base_ref[:, cols] = own_ref[:, cols] + part

        forward(stacked(got_pair_ref[...]), high_up, low_up, store)


def even_kernel(base_ref, got_ref, after_ref, field_ref):
    del after_ref

    @pl.when(jnp.logical_not(is_odd()))
    def _():
        field_ref[...] = base_ref[...] + got_ref[...]


def odd_kernel(sign, own_ref, got_pair_ref, got_ref, high_in, low_in, high_up, low_up, after_ref, field_ref, cross_ref):
    del after_ref

    @pl.when(is_odd())
    def _():
        tile = tile_of(own_ref.shape[1])

        def keep(start, part):
            cols = pl.ds(start, tile)
            field_ref[:, cols] = own_ref[:, cols] + sign * (got_pair_ref[:, cols] + part)

        def send(start, part):
            cross_ref[:, pl.ds(start, tile)] = part

        forward(stacked(got_ref[...]), high_up, low_up, keep)
        coupling(stacked(field_ref[...]), high_in, low_in, send)


def couple_even(field_ref, high_in, low_in, pair_ref):
    tile = tile_of(field_ref.shape[1])

    def send(start, part):
        pair_ref[:, pl.ds(start, tile)] = part

    coupling(stacked(field_ref[...]), high_in, low_in, send)


def merge_kernel(even_ref, odd_ref, high_in, low_in, field_ref, pair_ref):
    @pl.when(is_odd())
    def _():
        field_ref[...] = odd_ref[...]
        pair_ref[...] = odd_ref[...]

    @pl.when(jnp.logical_not(is_odd()))
    def _():
        field_ref[...] = even_ref[...]
        couple_even(field_ref, high_in, low_in, pair_ref)


def join_kernel(sign, base_ref, got_ref, odd_ref, high_in, low_in, field_ref, pair_ref):
    @pl.when(is_odd())
    def _():
        field_ref[...] = odd_ref[...]
        pair_ref[...] = odd_ref[...]

    @pl.when(jnp.logical_not(is_odd()))
    def _():
        field_ref[...] = base_ref[...] + sign * got_ref[...]
        couple_even(field_ref, high_in, low_in, pair_ref)


def reduce_kernel(field_ref, own_ref, got_pair_ref, got_up_ref, one_ref, two_ref, three_ref, out_ref):
    traits = field_ref.shape[0]
    lower = jnp.where(is_odd(), got_pair_ref[...], got_up_ref[...])
    last = moment(field_ref[...], own_ref[...] + 2.0 * lower)
    lane = lax.broadcasted_iota(jnp.int32, (traits, 128), 1)
    parts = (
        one_ref[:, 0:1],
        two_ref[:, 1:2],
        two_ref[:, 0:1],
        three_ref[:, 1:2],
        three_ref[:, 0:1],
        last,
    )
    table = jnp.zeros((traits, 128), F32)
    for index, part in enumerate(parts):
        table = jnp.where(lane == index, part, table)
    lanes = out_ref.shape[2]
    if lanes > traits:
        table = jnp.concatenate([table, jnp.zeros((lanes - traits, 128), F32)], axis=0)
    rows = jnp.transpose(table)[:MOMENT_ROWS]
    for index in range(out_ref.shape[0]):
        out_ref[index] = rows


def coefficients(moments, shift):
    def inner(left, right):
        total = None
        for i, a in enumerate(left):
            for j, b in enumerate(right):
                term = (a * b) * moments[i + j]
                total = term if total is None else total + term
        return total

    one = jnp.ones_like(shift)
    zero = jnp.zeros_like(shift)
    residual, direction, gain = [one], [one], []
    norm_now = moments[0]
    for step in range(ITERS):
        image = [shift * a + b for a, b in zip(direction + [zero], [zero] + direction)]
        alpha = norm_now / inner(direction, image)
        gain = [a + alpha * b for a, b in zip(gain + [zero], direction)]
        residual = [a - alpha * b for a, b in zip(residual + [zero], image)]
        if step + 1 < ITERS:
            norm_next = inner(residual, residual)
            ratio = norm_next / norm_now
            direction = [a + ratio * b for a, b in zip(residual, direction + [zero])]
            norm_now = norm_next
    return gain, residual


def weights_kernel(table_ref, shrinkage_ref, weights_ref):
    sums = jnp.sum(table_ref[...], axis=0)
    traits, lanes = weights_ref.shape[0], sums.shape[1]
    shift = 1.0 + shrinkage_ref[...]
    moments = [sums[i : i + 1, :traits] for i in range(2 * ITERS)]
    gain, residual = coefficients(moments, shift)
    row = lax.broadcasted_iota(jnp.int32, (lanes, traits), 0)
    table = jnp.zeros((lanes, traits), F32)
    for index, part in enumerate(gain + residual):
        table = jnp.where(row == index, part, table)
    weights_ref[...] = jnp.transpose(table)


def final_kernel(
    weights_ref, start_ref, zero_ref, one_ref, two_ref, own_ref, got_pair_ref, got_down_ref, got_up_ref,
    high_up, low_up, solution_ref, residual_ref,
):
    tile = tile_of(own_ref.shape[1])
    weights = [weights_ref[:, i : i + 1] for i in range(2 * ITERS + 1)]
    gain, residual = weights[:ITERS], weights[ITERS:]
    odd = is_odd()
    upper = jnp.where(odd, got_down_ref[...], got_pair_ref[...])
    lower = jnp.where(odd, got_pair_ref[...], got_up_ref[...])
    zero, one, two = zero_ref[...], one_ref[...], two_ref[...]
    solution_ref[...] = start_ref[...] + gain[0] * zero + gain[1] * one + gain[2] * two
    base = residual[0] * zero + residual[1] * one + residual[2] * two + residual[3] * (own_ref[...] + lower)

    def store(start, part):
        residual_ref[:, pl.ds(start, tile)] = base[:, start : start + tile] + residual[3] * part

    forward(stacked(upper), high_up, low_up, store)


def call(kernel, out, *args, spaces=None, scratch=(), limit=12, aliases=None, keep=True, flops=0):
    spaces = spaces or {}
    places = [spaces.get(i, VMEM) for i in range(len(args))]
    args = [
        arg if place is pltpu.SMEM else pltpu.with_memory_space_constraint(arg, place)
        for arg, place in zip(args, places)
    ]
    make = VMEM if keep else jax.ShapeDtypeStruct
    return pl.pallas_call(
        kernel,
        out_shape=[make(shape, dtype) for shape, dtype in out],
        in_specs=[pl.BlockSpec(memory_space=place) for place in places],
        out_specs=[pl.BlockSpec(memory_space=VMEM) for _ in out],
        scratch_shapes=scratch,
        input_output_aliases=aliases or {},
        cost_estimate=pl.CostEstimate(flops=flops, bytes_accessed=0, transcendentals=0) if flops else None,
        compiler_params=pltpu.CompilerParams(vmem_limit_bytes=limit * 1024 * 1024),
    )(*args)


def on_device(local_block, next_block, shrinkage, marginal, warm_start):
    count = lax.axis_size("snp")
    traits, size = warm_start.shape
    field = ((traits, size), F32)
    table = ((traits, 128), F32)
    matrix = ((size, size), BF16)
    work = 6 * traits * size * size
    copies = (
        pltpu.VMEM((size, size), F32),
        pltpu.VMEM((traits, size), F32),
        pltpu.SemaphoreType.DMA((size // tile_of(size) + 1,)),
    )
    on_chip = [(i, i ^ 1) for i in range(count) if i ^ 1 < count]
    downward = [(i + 1, i) for i in range(1, count - 1, 2)]
    upward = [(i, i + 1) for i in range(1, count - 1, 2)]

    def shift(value, route):
        return lax.ppermute(value, "snp", route)

    def run(kernel, out, *args, **rest):
        return call(kernel, out, *args, **rest)

    hbm = pltpu.HBM
    ridge = shrinkage.reshape(1, traits)
    down = shift(warm_start, downward)
    high_n, low_n, cross = run(
        begin_odd_kernel, [matrix, matrix, field], next_block, warm_start,
        spaces={0: hbm, 1: hbm}, scratch=copies, flops=work,
    )
    up = shift(cross, upward)
    high_n, low_n, high_l, low_l, own, pair = run(
        begin_even_kernel, [matrix, matrix, matrix, matrix, field, field],
        next_block, local_block, warm_start, high_n, low_n,
        spaces={0: hbm}, scratch=copies[::2], aliases={3: 0, 4: 1}, flops=work,
    )
    got_pair = shift(pair, on_chip)
    rest, high_up, low_up = run(
        prepare_odd_kernel, [field, matrix, matrix],
        own, warm_start, marginal, ridge, high_n, low_n, flops=work,
    )
    odd = functools.partial(odd_kernel, -1.0)
    odd_field, cross = run(odd, [field, field], rest, got_pair, down, high_n, low_n, high_up, low_up, ridge, flops=work)
    next_up = shift(cross, upward)
    high_l, low_l, high_up, low_up, base = run(
        prepare_even_kernel, [matrix, matrix, matrix, matrix, field],
        local_block, warm_start, marginal, ridge, got_pair, high_n, low_n,
        high_l, low_l, high_up, low_up, odd_field,
        aliases={7: 0, 8: 1, 9: 2, 10: 3}, flops=work,
    )
    join = functools.partial(join_kernel, -1.0)
    merged, pair = run(join, [field, field], base, up, odd_field, high_n, low_n, flops=work)
    up = next_up
    fields, tables = [merged], []
    odd, join = functools.partial(odd_kernel, 1.0), functools.partial(join_kernel, 1.0)
    for step in range(2, ITERS + 2):
        got_pair = shift(pair, on_chip)
        if step % 2 == 0:
            down = shift(merged, downward)
        before = fields[-2:-1]
        kernel = own_kernel if before else functools.partial(own_kernel, None)
        own, part = run(kernel, [field, table], *before, merged, high_l, low_l, flops=work)
        tables.append(part)
        if step > ITERS:
            break
        (base,) = run(pair_kernel, [field], own, got_pair, high_up, low_up, flops=work)
        if step % 2 == 0:
            (even_field,) = run(even_kernel, [field], base, up, ridge, flops=work)
            next_down = shift(even_field, downward)
            odd_field, cross = run(
                odd, [field, field],
                own, got_pair, down, high_n, low_n, high_up, low_up, even_field, flops=work,
            )
            up = shift(cross, upward)
            down = next_down
            merged, pair = run(merge_kernel, [field, field], even_field, odd_field, high_n, low_n, flops=work)
        else:
            odd_field, cross = run(
                odd, [field, field],
                own, got_pair, down, high_n, low_n, high_up, low_up, base, flops=work,
            )
            next_up = shift(cross, upward)
            merged, pair = run(join, [field, field], base, up, odd_field, high_n, low_n, flops=work)
            up = next_up
        fields.append(merged)
    lanes = -(-traits // 128) * 128
    (moments,) = run(reduce_kernel, [((count, MOMENT_ROWS, lanes), F32)], fields[-1], own, got_pair, up, *tables)
    moments = lax.all_to_all(moments, "snp", 0, 0)
    (weights,) = run(weights_kernel, [table], moments, ridge)
    return tuple(
        run(
            final_kernel, [field, field],
            weights, warm_start, *fields, own, got_pair, down, up, high_up, low_up,
            keep=False,
        )
    )


def solution(mesh):
    return jax.shard_map(
        on_device,
        mesh=mesh,
        in_specs=(
            P(("parts", "snp"), None),
            P(("parts", "snp"), None),
            P(),
            P(None, ("parts", "snp")),
            P(None, ("parts", "snp")),
        ),
        out_specs=(P(None, ("parts", "snp")), P(None, ("parts", "snp"))),
        check_vma=False,
    )
```

```python
import functools

import jax
import jax.numpy as jnp
from jax import lax
from jax.experimental import pallas as pl
from jax.experimental.pallas import tpu as pltpu
from jax.sharding import PartitionSpec as P


ITERS = 3
F32 = jnp.float32
BF16 = jnp.bfloat16
VMEM = pltpu.VMEM
MOMENT_ROWS = 8


def tile_of(size):
    return 256 if size % 256 == 0 else size


def is_odd():
    return lax.rem(lax.axis_index("snp"), 2) == 1


def halves(x):
    high = x.astype(BF16)
    return high, (x - high.astype(F32)).astype(BF16)


def dot(left, right):
    return jnp.dot(left, right, preferred_element_type=F32)


def product(both, right_high, right_low):
    rows = both.shape[0] // 2
    main = dot(both, right_high)
    return main[:rows] + main[rows:] + dot(both[:rows], right_low)


def stacked(field):
    return jnp.concatenate(halves(field), axis=0)


def coupling(both, high, low, store):
    size = high.shape[0]
    tile = tile_of(size)
    for start in range(0, size, tile):
        rows, cols = pl.ds(start, size - start), pl.ds(start, tile)
        store(start, product(both[:, start:], high[rows, cols], low[rows, cols]))


def forward(both, high, low, store):
    size = high.shape[0]
    tile = tile_of(size)
    for start in range(0, size, tile):
        rows, cols = pl.ds(0, start + tile), pl.ds(start, tile)
        store(start, product(both[:, : start + tile], high[rows, cols], low[rows, cols]))


def adding(total_ref):
    def store(start, part):
        tile = part.shape[1] - start
        if start:
            total_ref[:, pl.ds(0, start)] = total_ref[:, pl.ds(0, start)] + part[:, :start]
        total_ref[:, pl.ds(start, tile)] = part[:, start:]

    return store


def load(source_ref, parts, raw, sems):
    copies = [
        pltpu.make_async_copy(source_ref.at[part], raw.at[part], sems.at[index]) for index, part in enumerate(parts)
    ]
    for copy in copies:
        copy.start()
    return copies


def take_next(next_ref, field_ref, high_ref, low_ref, out_ref, raw, sems, field=None):
    size = raw.shape[0]
    tile = tile_of(size)
    starts = list(range(0, size, tile))
    parts = [(pl.ds(start, tile), pl.ds(0, start + tile)) for start in starts]
    if field is not None:
        ours = pltpu.make_async_copy(field_ref, field, sems.at[len(starts)])
        ours.start()
    copies = load(next_ref, parts, raw, sems)
    store = adding(out_ref)
    if field is not None:
        ours.wait()
        field_ref = field
    for start, part, copy in zip(starts, parts, copies):
        copy.wait()
        high, low = halves(raw[part])
        high_ref[part] = high
        low_ref[part] = low
        store(start, product(stacked(field_ref[:, pl.ds(start, tile)]), high, low))


def take_local(local_ref, field_ref, high_ref, low_ref, out_ref):
    size = local_ref.shape[0]
    tile = tile_of(size)
    both = stacked(field_ref[...])
    for start in range(0, size, tile):
        rows = pl.ds(start, tile)
        row = lax.broadcasted_iota(jnp.int32, (tile, size), 0) + start
        col = lax.broadcasted_iota(jnp.int32, (tile, size), 1)
        high, low = halves(local_ref[rows, :] - jnp.where(row == col, 1.0, 0.0))
        high_ref[rows, :] = high
        low_ref[rows, :] = low
        done = product(both[:, start : start + tile], high, low)
        out_ref[...] = done if start == 0 else out_ref[...] + done


def begin_odd_kernel(next_ref, start_ref, high_n, low_n, cross_ref, raw, field, sems):
    @pl.when(is_odd())
    def _():
        take_next(next_ref, start_ref, high_n, low_n, cross_ref, raw, sems, field)

    @pl.when(jnp.logical_not(is_odd()))
    def _():
        copy = pltpu.make_async_copy(start_ref, cross_ref, sems.at[0])
        copy.start()
        copy.wait()


def begin_even_kernel(
    next_ref, local_ref, start_ref, high_n_in, low_n_in,
    high_n, low_n, high_l, low_l, own_ref, pair_ref, raw, sems,
):
    del high_n_in, low_n_in

    @pl.when(is_odd())
    def _():
        take_local(local_ref, start_ref, high_l, low_l, own_ref)
        pair_ref[...] = start_ref[...]

    @pl.when(jnp.logical_not(is_odd()))
    def _():
        take_next(next_ref, start_ref, high_n, low_n, pair_ref, raw, sems)


def flip(high_in, low_in, high_ref, low_ref):
    size = high_in.shape[0]
    tile = tile_of(size)
    for row in range(0, size, tile):
        for col in range(0, row + tile, tile):
            source, target = (pl.ds(row, tile), pl.ds(col, tile)), (pl.ds(col, tile), pl.ds(row, tile))
            high_ref[target] = jnp.transpose(high_in[source])
            low_ref[target] = jnp.transpose(low_in[source])


def ridge_column(shrinkage_ref):
    traits = shrinkage_ref.shape[1]
    here = lax.broadcasted_iota(jnp.int32, (traits, traits), 0) == lax.broadcasted_iota(jnp.int32, (traits, traits), 1)
    return 1.0 + jnp.sum(jnp.where(here, shrinkage_ref[...], 0.0), axis=1, keepdims=True)


def prepare_kernel(
    own_ref, local_ref, start_ref, marginal_ref, shrinkage_ref, got_pair_ref, high_n, low_n, high_l_in, low_l_in,
    high_l, low_l, high_up, low_up, base_ref,
):
    del high_l_in, low_l_in
    flip(high_n, low_n, high_up, low_up)

    @pl.when(is_odd())
    def _():
        rest = marginal_ref[...] - ridge_column(shrinkage_ref) * start_ref[...]
        base_ref[...] = rest - own_ref[...] - got_pair_ref[...]

    @pl.when(jnp.logical_not(is_odd()))
    def _():
        take_local(local_ref, start_ref, high_l, low_l, base_ref)
        base_ref[...] = marginal_ref[...] - ridge_column(shrinkage_ref) * start_ref[...] - base_ref[...]
        tile = tile_of(base_ref.shape[1])

        def store(start, part):
            cols = pl.ds(start, tile)
            base_ref[:, cols] = base_ref[:, cols] - part

        forward(stacked(got_pair_ref[...]), high_up, low_up, store)


def field_then_coupling(base, got, high_in, low_in, high_up, low_up, keep, send):
    size = high_up.shape[0]
    tile = tile_of(size)
    both = stacked(got)
    done = []
    waiting = None

    def couple(start):
        rows, cols = pl.ds(start, size - start), pl.ds(start, tile)
        send(start, product(jnp.concatenate(done, axis=1), high_in[rows, cols], low_in[rows, cols]))

    for start in reversed(range(0, size, tile)):
        rows, cols = pl.ds(0, start + tile), pl.ds(start, tile)
        part = product(both[:, : start + tile], high_up[rows, cols], low_up[rows, cols])
        if waiting is not None:
            couple(waiting)
        field = base(cols, part)
        keep(cols, field)
        done.insert(0, stacked(field))
        waiting = start
    couple(waiting)


def moment(left, right):
    return jnp.sum(left * right, axis=1, keepdims=True)


def own_kernel(before_ref, field_ref, high_ref, low_ref, own_ref, moments_ref):
    field = field_ref[...]
    own_ref[...] = product(stacked(field), high_ref[...], low_ref[...])
    lane = lax.broadcasted_iota(jnp.int32, moments_ref.shape, 1)
    cross = 0.0 if before_ref is None else moment(before_ref[...], field)
    moments_ref[...] = jnp.where(lane == 0, moment(field, field), jnp.where(lane == 1, cross, 0.0))


def pair_kernel(own_ref, got_pair_ref, high_up, low_up, base_ref):
    @pl.when(jnp.logical_not(is_odd()))
    def _():
        tile = tile_of(own_ref.shape[1])

        def store(start, part):
            cols = pl.ds(start, tile)
            base_ref[:, cols] = own_ref[:, cols] + part

        forward(stacked(got_pair_ref[...]), high_up, low_up, store)


def even_kernel(base_ref, got_ref, after_ref, field_ref):
    del after_ref

    @pl.when(jnp.logical_not(is_odd()))
    def _():
        field_ref[...] = base_ref[...] + got_ref[...]


def odd_kernel(own_ref, got_pair_ref, got_ref, high_in, low_in, high_up, low_up, after_ref, field_ref, cross_ref):
    del after_ref

    @pl.when(is_odd())
    def _():
        tile = tile_of(own_ref.shape[1])

        def base(cols, part):
            return own_ref[:, cols] + (got_pair_ref[:, cols] + part)

        def keep(cols, field):
            field_ref[:, cols] = field

        def send(start, part):
            cross_ref[:, pl.ds(start, tile)] = part

        field_then_coupling(base, got_ref[...], high_in, low_in, high_up, low_up, keep, send)


def first_kernel(base_ref, got_ref, high_in, low_in, high_up, low_up, field_ref, pair_ref, cross_ref):
    tile = tile_of(base_ref.shape[1])

    @pl.when(is_odd())
    def _():
        def base(cols, part):
            return base_ref[:, cols] - part

        def keep(cols, field):
            field_ref[:, cols] = field
            pair_ref[:, cols] = field

        def send(start, part):
            cross_ref[:, pl.ds(start, tile)] = part

        field_then_coupling(base, got_ref[...], high_in, low_in, high_up, low_up, keep, send)

    @pl.when(jnp.logical_not(is_odd()))
    def _():
        field_ref[...] = base_ref[...] - got_ref[...]
        couple_even(field_ref, high_in, low_in, pair_ref)


def couple_even(field_ref, high_in, low_in, pair_ref):
    tile = tile_of(field_ref.shape[1])

    def send(start, part):
        pair_ref[:, pl.ds(start, tile)] = part

    coupling(stacked(field_ref[...]), high_in, low_in, send)


def merge_kernel(even_ref, odd_ref, high_in, low_in, field_ref, pair_ref):
    @pl.when(is_odd())
    def _():
        field_ref[...] = odd_ref[...]
        pair_ref[...] = odd_ref[...]

    @pl.when(jnp.logical_not(is_odd()))
    def _():
        field_ref[...] = even_ref[...]
        couple_even(field_ref, high_in, low_in, pair_ref)


def join_kernel(base_ref, got_ref, odd_ref, high_in, low_in, field_ref, pair_ref):
    @pl.when(is_odd())
    def _():
        field_ref[...] = odd_ref[...]
        pair_ref[...] = odd_ref[...]

    @pl.when(jnp.logical_not(is_odd()))
    def _():
        field_ref[...] = base_ref[...] + got_ref[...]
        couple_even(field_ref, high_in, low_in, pair_ref)


def reduce_kernel(field_ref, own_ref, got_pair_ref, got_up_ref, one_ref, two_ref, three_ref, out_ref):
    traits = field_ref.shape[0]
    lower = jnp.where(is_odd(), got_pair_ref[...], got_up_ref[...])
    last = moment(field_ref[...], own_ref[...] + 2.0 * lower)
    lane = lax.broadcasted_iota(jnp.int32, (traits, 128), 1)
    parts = (
        one_ref[:, 0:1],
        two_ref[:, 1:2],
        two_ref[:, 0:1],
        three_ref[:, 1:2],
        three_ref[:, 0:1],
        last,
    )
    table = jnp.zeros((traits, 128), F32)
    for index, part in enumerate(parts):
        table = jnp.where(lane == index, part, table)
    lanes = out_ref.shape[2]
    if lanes > traits:
        table = jnp.concatenate([table, jnp.zeros((lanes - traits, 128), F32)], axis=0)
    rows = jnp.transpose(table)[:MOMENT_ROWS]
    for index in range(out_ref.shape[0]):
        out_ref[index] = rows


def coefficients(moments, shift):
    def inner(left, right):
        total = None
        for i, a in enumerate(left):
            for j, b in enumerate(right):
                term = (a * b) * moments[i + j]
                total = term if total is None else total + term
        return total

    one = jnp.ones_like(shift)
    zero = jnp.zeros_like(shift)
    residual, direction, gain = [one], [one], []
    norm_now = moments[0]
    for step in range(ITERS):
        image = [shift * a + b for a, b in zip(direction + [zero], [zero] + direction)]
        alpha = norm_now / inner(direction, image)
        gain = [a + alpha * b for a, b in zip(gain + [zero], direction)]
        residual = [a - alpha * b for a, b in zip(residual + [zero], image)]
        if step + 1 < ITERS:
            norm_next = inner(residual, residual)
            ratio = norm_next / norm_now
            direction = [a + ratio * b for a, b in zip(residual, direction + [zero])]
            norm_now = norm_next
    return gain, residual


def weights_kernel(table_ref, shrinkage_ref, weights_ref):
    sums = jnp.sum(table_ref[...], axis=0)
    traits, lanes = weights_ref.shape[0], sums.shape[1]
    shift = 1.0 + shrinkage_ref[...]
    moments = [sums[i : i + 1, :traits] for i in range(2 * ITERS)]
    gain, residual = coefficients(moments, shift)
    row = lax.broadcasted_iota(jnp.int32, (lanes, traits), 0)
    table = jnp.zeros((lanes, traits), F32)
    for index, part in enumerate(gain + residual):
        table = jnp.where(row == index, part, table)
    weights_ref[...] = jnp.transpose(table)


def final_kernel(
    weights_ref, start_ref, zero_ref, one_ref, two_ref, own_ref, got_pair_ref, got_down_ref, got_up_ref,
    high_up, low_up, solution_ref, residual_ref, solution, residual, sems,
):
    size = own_ref.shape[1]
    tile = tile_of(size)
    weights = [weights_ref[:, i : i + 1] for i in range(2 * ITERS + 1)]
    gain, rest = weights[:ITERS], weights[ITERS:]
    odd = is_odd()
    copies = []

    def write(held, target, cols):
        copies.append(pltpu.make_async_copy(held.at[:, cols], target.at[:, cols], sems.at[len(copies)]))
        copies[-1].start()

    for start in range(0, size, tile):
        cols = pl.ds(start, tile)
        steps = gain[0] * zero_ref[:, cols] + gain[1] * one_ref[:, cols] + gain[2] * two_ref[:, cols]
        solution[:, cols] = start_ref[:, cols] + steps
        write(solution, solution_ref, cols)
    upper = stacked(jnp.where(odd, got_down_ref[...], got_pair_ref[...]))
    for start in range(0, size, tile):
        rows, cols = pl.ds(0, start + tile), pl.ds(start, tile)
        part = product(upper[:, : start + tile], high_up[rows, cols], low_up[rows, cols])
        lower = jnp.where(odd, got_pair_ref[:, cols], got_up_ref[:, cols])
        steps = rest[0] * zero_ref[:, cols] + rest[1] * one_ref[:, cols] + rest[2] * two_ref[:, cols]
        residual[:, cols] = steps + rest[3] * (own_ref[:, cols] + lower + part)
        write(residual, residual_ref, cols)
    for copy in copies:
        copy.wait()


def call(kernel, out, *args, spaces=None, scratch=(), limit=12, aliases=None, keep=True, flops=0):
    spaces = spaces or {}
    places = [spaces.get(i, VMEM) for i in range(len(args))]
    args = [
        arg if place is pltpu.SMEM else pltpu.with_memory_space_constraint(arg, place)
        for arg, place in zip(args, places)
    ]
    make = VMEM if keep else jax.ShapeDtypeStruct
    return pl.pallas_call(
        kernel,
        out_shape=[make(shape, dtype) for shape, dtype in out],
        in_specs=[pl.BlockSpec(memory_space=place) for place in places],
        out_specs=[pl.BlockSpec(memory_space=VMEM if keep else pltpu.HBM) for _ in out],
        scratch_shapes=scratch,
        input_output_aliases=aliases or {},
        cost_estimate=pl.CostEstimate(flops=flops, bytes_accessed=0, transcendentals=0) if flops else None,
        compiler_params=pltpu.CompilerParams(vmem_limit_bytes=limit * 1024 * 1024),
    )(*args)


def on_device(local_block, next_block, shrinkage, marginal, warm_start):
    count = lax.axis_size("snp")
    traits, size = warm_start.shape
    field = ((traits, size), F32)
    table = ((traits, 128), F32)
    matrix = ((size, size), BF16)
    work = 6 * traits * size * size
    copies = (
        pltpu.VMEM((size, size), F32),
        pltpu.VMEM((traits, size), F32),
        pltpu.SemaphoreType.DMA((size // tile_of(size) + 1,)),
    )
    on_chip = [(i, i ^ 1) for i in range(count) if i ^ 1 < count]
    off_chip = [(i, ((i - 1) ^ 1) + 1) for i in range(1, count) if ((i - 1) ^ 1) + 1 < count]
    downward = [(i + 1, i) for i in range(1, count - 1, 2)]
    upward = [(i, i + 1) for i in range(1, count - 1, 2)]

    def shift(value, route):
        return lax.ppermute(value, "snp", route)

    def run(kernel, out, *args, **rest):
        return call(kernel, out, *args, **rest)

    hbm = pltpu.HBM
    ridge = shrinkage.reshape(1, traits)
    high_n, low_n, cross = run(
        begin_odd_kernel, [matrix, matrix, field], next_block, warm_start,
        spaces={0: hbm, 1: hbm}, scratch=copies, flops=work,
    )
    got = shift(cross, off_chip)
    high_n, low_n, high_l, low_l, own, pair = run(
        begin_even_kernel, [matrix, matrix, matrix, matrix, field, field],
        next_block, local_block, warm_start, high_n, low_n,
        spaces={0: hbm}, scratch=copies[::2], aliases={3: 0, 4: 1}, flops=work,
    )
    got_pair = shift(pair, on_chip)
    high_l, low_l, high_up, low_up, base = run(
        prepare_kernel, [matrix, matrix, matrix, matrix, field],
        own, local_block, warm_start, marginal, ridge, got_pair, high_n, low_n, high_l, low_l,
        aliases={8: 0, 9: 1}, flops=work,
    )
    merged, pair, cross = run(
        first_kernel, [field, field, field], base, got, high_n, low_n, high_up, low_up, flops=work
    )
    up = shift(cross, upward)
    fields, tables = [merged], []
    for step in range(2, ITERS + 2):
        got_pair = shift(pair, on_chip)
        if step % 2 == 0:
            down = shift(merged, downward)
        before = fields[-2:-1]
        kernel = own_kernel if before else functools.partial(own_kernel, None)
        own, part = run(kernel, [field, table], *before, merged, high_l, low_l, flops=work)
        tables.append(part)
        if step > ITERS:
            break
        (base,) = run(pair_kernel, [field], own, got_pair, high_up, low_up, flops=work)
        if step % 2 == 0:
            (even_field,) = run(even_kernel, [field], base, up, ridge, flops=work)
            next_down = shift(even_field, downward)
            odd_field, cross = run(
                odd_kernel, [field, field],
                own, got_pair, down, high_n, low_n, high_up, low_up, even_field, flops=work,
            )
            up = shift(cross, upward)
            down = next_down
            merged, pair = run(merge_kernel, [field, field], even_field, odd_field, high_n, low_n, flops=work)
        else:
            odd_field, cross = run(
                odd_kernel, [field, field],
                own, got_pair, down, high_n, low_n, high_up, low_up, base, flops=work,
            )
            next_up = shift(cross, upward)
            merged, pair = run(join_kernel, [field, field], base, up, odd_field, high_n, low_n, flops=work)
            up = next_up
        fields.append(merged)
    lanes = -(-traits // 128) * 128
    (moments,) = run(reduce_kernel, [((count, MOMENT_ROWS, lanes), F32)], fields[-1], own, got_pair, up, *tables)
    moments = lax.all_to_all(moments, "snp", 0, 0)
    (weights,) = run(weights_kernel, [table], moments, ridge)
    return tuple(
        run(
            final_kernel, [field, field],
            weights, warm_start, *fields, own, got_pair, down, up, high_up, low_up,
            keep=False,
            scratch=(
                pltpu.VMEM((traits, size), F32),
                pltpu.VMEM((traits, size), F32),
                pltpu.SemaphoreType.DMA((2 * (size // tile_of(size)),)),
            ),
        )
    )


def solution(mesh):
    return jax.shard_map(
        on_device,
        mesh=mesh,
        in_specs=(
            P(("parts", "snp"), None),
            P(("parts", "snp"), None),
            P(),
            P(None, ("parts", "snp")),
            P(None, ("parts", "snp")),
        ),
        out_specs=(P(None, ("parts", "snp")), P(None, ("parts", "snp"))),
        check_vma=False,
    )
```

```python
import functools

import jax
import jax.numpy as jnp
from jax import lax
from jax.experimental import pallas as pl
from jax.experimental.pallas import tpu as pltpu
from jax.sharding import PartitionSpec as P


ITERS = 3
F32 = jnp.float32
BF16 = jnp.bfloat16
VMEM = pltpu.VMEM
MOMENT_ROWS = 8


def tile_of(size):
    return 256 if size % 256 == 0 else size


def is_odd():
    return lax.rem(lax.axis_index("snp"), 2) == 1


def halves(x):
    high = x.astype(BF16)
    return high, (x - high.astype(F32)).astype(BF16)


def dot(left, right):
    return jnp.dot(left, right, preferred_element_type=F32)


def product(both, right_high, right_low):
    rows = both.shape[0] // 2
    main = dot(both, right_high)
    return main[:rows] + main[rows:] + dot(both[:rows], right_low)


def stacked(field):
    return jnp.concatenate(halves(field), axis=0)


def coupling(both, high, low, store):
    size = high.shape[0]
    tile = tile_of(size)
    for start in range(0, size, tile):
        rows, cols = pl.ds(start, size - start), pl.ds(start, tile)
        store(start, product(both[:, start:], high[rows, cols], low[rows, cols]))


def forward(both, high, low, store):
    size = high.shape[0]
    tile = tile_of(size)
    for start in range(0, size, tile):
        rows, cols = pl.ds(0, start + tile), pl.ds(start, tile)
        store(start, product(both[:, : start + tile], high[rows, cols], low[rows, cols]))


def adding(total_ref):
    def store(start, part):
        tile = part.shape[1] - start
        if start:
            total_ref[:, pl.ds(0, start)] = total_ref[:, pl.ds(0, start)] + part[:, :start]
        total_ref[:, pl.ds(start, tile)] = part[:, start:]

    return store


def load(source_ref, parts, raw, sems):
    copies = [
        pltpu.make_async_copy(source_ref.at[part], raw.at[part], sems.at[index]) for index, part in enumerate(parts)
    ]
    for copy in copies:
        copy.start()
    return copies


def take_next(next_ref, field_ref, high_ref, low_ref, out_ref, raw, sems, field=None):
    size = raw.shape[0]
    tile = tile_of(size)
    starts = list(range(0, size, tile))
    parts = [(pl.ds(start, tile), pl.ds(0, start + tile)) for start in starts]
    if field is not None:
        ours = pltpu.make_async_copy(field_ref, field, sems.at[len(starts)])
        ours.start()
    copies = load(next_ref, parts, raw, sems)
    store = adding(out_ref)
    if field is not None:
        ours.wait()
        field_ref = field
    for start, part, copy in zip(starts, parts, copies):
        copy.wait()
        high, low = halves(raw[part])
        high_ref[part] = high
        low_ref[part] = low
        store(start, product(stacked(field_ref[:, pl.ds(start, tile)]), high, low))


def take_local(local_ref, field_ref, high_ref, low_ref, out_ref):
    size = local_ref.shape[0]
    tile = tile_of(size)
    both = stacked(field_ref[...])
    for start in range(0, size, tile):
        rows = pl.ds(start, tile)
        row = lax.broadcasted_iota(jnp.int32, (tile, size), 0) + start
        col = lax.broadcasted_iota(jnp.int32, (tile, size), 1)
        high, low = halves(local_ref[rows, :] - jnp.where(row == col, 1.0, 0.0))
        high_ref[rows, :] = high
        low_ref[rows, :] = low
        done = product(both[:, start : start + tile], high, low)
        out_ref[...] = done if start == 0 else out_ref[...] + done


def begin_odd_kernel(next_ref, start_ref, high_n, low_n, cross_ref, raw, field, sems):
    @pl.when(is_odd())
    def _():
        take_next(next_ref, start_ref, high_n, low_n, cross_ref, raw, sems, field)


def local_odd_kernel(local_ref, start_ref, after_ref, high_l, low_l, own_ref, pair_ref):
    del after_ref

    @pl.when(is_odd())
    def _():
        take_local(local_ref, start_ref, high_l, low_l, own_ref)
        pair_ref[...] = start_ref[...]


def begin_even_kernel(next_ref, start_ref, high_n_in, low_n_in, pair_in, high_n, low_n, pair_ref, raw, sems):
    del high_n_in, low_n_in, pair_in

    @pl.when(jnp.logical_not(is_odd()))
    def _():
        take_next(next_ref, start_ref, high_n, low_n, pair_ref, raw, sems)


def flip(high_in, low_in, high_ref, low_ref):
    size = high_in.shape[0]
    tile = tile_of(size)
    for row in range(0, size, tile):
        for col in range(0, row + tile, tile):
            source, target = (pl.ds(row, tile), pl.ds(col, tile)), (pl.ds(col, tile), pl.ds(row, tile))
            high_ref[target] = jnp.transpose(high_in[source])
            low_ref[target] = jnp.transpose(low_in[source])


def ridge_column(shrinkage_ref):
    traits = shrinkage_ref.shape[1]
    here = lax.broadcasted_iota(jnp.int32, (traits, traits), 0) == lax.broadcasted_iota(jnp.int32, (traits, traits), 1)
    return 1.0 + jnp.sum(jnp.where(here, shrinkage_ref[...], 0.0), axis=1, keepdims=True)


def prepare_odd_kernel(own_ref, start_ref, marginal_ref, shrinkage_ref, high_n, low_n, rest_ref, high_up, low_up):
    @pl.when(is_odd())
    def _():
        rest_ref[...] = marginal_ref[...] - ridge_column(shrinkage_ref) * start_ref[...] - own_ref[...]
        flip(high_n, low_n, high_up, low_up)


def prepare_even_kernel(
    local_ref, start_ref, marginal_ref, shrinkage_ref, got_pair_ref, high_n, low_n,
    high_l_in, low_l_in, high_up_in, low_up_in, after_ref,
    high_l, low_l, high_up, low_up, base_ref,
):
    del high_l_in, low_l_in, high_up_in, low_up_in, after_ref

    @pl.when(jnp.logical_not(is_odd()))
    def _():
        flip(high_n, low_n, high_up, low_up)
        take_local(local_ref, start_ref, high_l, low_l, base_ref)
        base_ref[...] = marginal_ref[...] - ridge_column(shrinkage_ref) * start_ref[...] - base_ref[...]
        tile = tile_of(base_ref.shape[1])

        def store(start, part):
            cols = pl.ds(start, tile)
            base_ref[:, cols] = base_ref[:, cols] - part

        forward(stacked(got_pair_ref[...]), high_up, low_up, store)


def moment(left, right):
    return jnp.sum(left * right, axis=1, keepdims=True)


def own_kernel(before_ref, field_ref, high_ref, low_ref, own_ref, moments_ref):
    field = field_ref[...]
    own_ref[...] = product(stacked(field), high_ref[...], low_ref[...])
    lane = lax.broadcasted_iota(jnp.int32, moments_ref.shape, 1)
    cross = 0.0 if before_ref is None else moment(before_ref[...], field)
    moments_ref[...] = jnp.where(lane == 0, moment(field, field), jnp.where(lane == 1, cross, 0.0))


def pair_kernel(own_ref, got_pair_ref, high_up, low_up, base_ref):
    @pl.when(jnp.logical_not(is_odd()))
    def _():
        tile = tile_of(own_ref.shape[1])

        def store(start, part):
            cols = pl.ds(start, tile)
            base_ref[:, cols] = own_ref[:, cols] + part

        forward(stacked(got_pair_ref[...]), high_up, low_up, store)


def even_kernel(base_ref, got_ref, after_ref, field_ref):
    del after_ref

    @pl.when(jnp.logical_not(is_odd()))
    def _():
        field_ref[...] = base_ref[...] + got_ref[...]


def odd_kernel(sign, own_ref, got_pair_ref, got_ref, high_in, low_in, high_up, low_up, after_ref, field_ref, cross_ref):
    del after_ref

    @pl.when(is_odd())
    def _():
        tile = tile_of(own_ref.shape[1])

        def keep(start, part):
            cols = pl.ds(start, tile)
            field_ref[:, cols] = own_ref[:, cols] + sign * (got_pair_ref[:, cols] + part)

        def send(start, part):
            cross_ref[:, pl.ds(start, tile)] = part

        forward(stacked(got_ref[...]), high_up, low_up, keep)
        coupling(stacked(field_ref[...]), high_in, low_in, send)


def couple_even(field_ref, high_in, low_in, pair_ref):
    tile = tile_of(field_ref.shape[1])

    def send(start, part):
        pair_ref[:, pl.ds(start, tile)] = part

    coupling(stacked(field_ref[...]), high_in, low_in, send)


def merge_kernel(even_ref, odd_ref, high_in, low_in, field_ref, pair_ref):
    @pl.when(is_odd())
    def _():
        field_ref[...] = odd_ref[...]
        pair_ref[...] = odd_ref[...]

    @pl.when(jnp.logical_not(is_odd()))
    def _():
        field_ref[...] = even_ref[...]
        couple_even(field_ref, high_in, low_in, pair_ref)


def join_kernel(sign, base_ref, got_ref, odd_ref, high_in, low_in, field_ref, pair_ref):
    @pl.when(is_odd())
    def _():
        field_ref[...] = odd_ref[...]
        pair_ref[...] = odd_ref[...]

    @pl.when(jnp.logical_not(is_odd()))
    def _():
        field_ref[...] = base_ref[...] + sign * got_ref[...]
        couple_even(field_ref, high_in, low_in, pair_ref)


def reduce_kernel(field_ref, own_ref, got_pair_ref, got_up_ref, one_ref, two_ref, three_ref, out_ref):
    traits = field_ref.shape[0]
    lower = jnp.where(is_odd(), got_pair_ref[...], got_up_ref[...])
    last = moment(field_ref[...], own_ref[...] + 2.0 * lower)
    lane = lax.broadcasted_iota(jnp.int32, (traits, 128), 1)
    parts = (
        one_ref[:, 0:1],
        two_ref[:, 1:2],
        two_ref[:, 0:1],
        three_ref[:, 1:2],
        three_ref[:, 0:1],
        last,
    )
    table = jnp.zeros((traits, 128), F32)
    for index, part in enumerate(parts):
        table = jnp.where(lane == index, part, table)
    lanes = out_ref.shape[2]
    if lanes > traits:
        table = jnp.concatenate([table, jnp.zeros((lanes - traits, 128), F32)], axis=0)
    rows = jnp.transpose(table)[:MOMENT_ROWS]
    for index in range(out_ref.shape[0]):
        out_ref[index] = rows


def coefficients(moments, shift):
    def inner(left, right):
        total = None
        for i, a in enumerate(left):
            for j, b in enumerate(right):
                term = (a * b) * moments[i + j]
                total = term if total is None else total + term
        return total

    one = jnp.ones_like(shift)
    zero = jnp.zeros_like(shift)
    residual, direction, gain = [one], [one], []
    norm_now = moments[0]
    for step in range(ITERS):
        image = [shift * a + b for a, b in zip(direction + [zero], [zero] + direction)]
        alpha = norm_now / inner(direction, image)
        gain = [a + alpha * b for a, b in zip(gain + [zero], direction)]
        residual = [a - alpha * b for a, b in zip(residual + [zero], image)]
        if step + 1 < ITERS:
            norm_next = inner(residual, residual)
            ratio = norm_next / norm_now
            direction = [a + ratio * b for a, b in zip(residual, direction + [zero])]
            norm_now = norm_next
    return gain, residual


def weights_kernel(table_ref, shrinkage_ref, weights_ref):
    sums = jnp.sum(table_ref[...], axis=0)
    traits, lanes = weights_ref.shape[0], sums.shape[1]
    shift = 1.0 + shrinkage_ref[...]
    moments = [sums[i : i + 1, :traits] for i in range(2 * ITERS)]
    gain, residual = coefficients(moments, shift)
    row = lax.broadcasted_iota(jnp.int32, (lanes, traits), 0)
    table = jnp.zeros((lanes, traits), F32)
    for index, part in enumerate(gain + residual):
        table = jnp.where(row == index, part, table)
    weights_ref[...] = jnp.transpose(table)


def final_kernel(
    weights_ref, start_ref, zero_ref, one_ref, two_ref, own_ref, got_pair_ref, got_down_ref, got_up_ref,
    high_up, low_up, solution_ref, residual_ref,
):
    tile = tile_of(own_ref.shape[1])
    weights = [weights_ref[:, i : i + 1] for i in range(2 * ITERS + 1)]
    gain, residual = weights[:ITERS], weights[ITERS:]
    odd = is_odd()
    upper = jnp.where(odd, got_down_ref[...], got_pair_ref[...])
    lower = jnp.where(odd, got_pair_ref[...], got_up_ref[...])
    zero, one, two = zero_ref[...], one_ref[...], two_ref[...]
    solution_ref[...] = start_ref[...] + gain[0] * zero + gain[1] * one + gain[2] * two
    base = residual[0] * zero + residual[1] * one + residual[2] * two + residual[3] * (own_ref[...] + lower)

    def store(start, part):
        residual_ref[:, pl.ds(start, tile)] = base[:, start : start + tile] + residual[3] * part

    forward(stacked(upper), high_up, low_up, store)


def call(kernel, out, *args, spaces=None, scratch=(), limit=12, aliases=None, keep=True, flops=0):
    spaces = spaces or {}
    places = [spaces.get(i, VMEM) for i in range(len(args))]
    args = [
        arg if place is pltpu.SMEM else pltpu.with_memory_space_constraint(arg, place)
        for arg, place in zip(args, places)
    ]
    make = VMEM if keep else jax.ShapeDtypeStruct
    return pl.pallas_call(
        kernel,
        out_shape=[make(shape, dtype) for shape, dtype in out],
        in_specs=[pl.BlockSpec(memory_space=place) for place in places],
        out_specs=[pl.BlockSpec(memory_space=VMEM) for _ in out],
        scratch_shapes=scratch,
        input_output_aliases=aliases or {},
        cost_estimate=pl.CostEstimate(flops=flops, bytes_accessed=0, transcendentals=0) if flops else None,
        compiler_params=pltpu.CompilerParams(vmem_limit_bytes=limit * 1024 * 1024),
    )(*args)


def on_device(local_block, next_block, shrinkage, marginal, warm_start):
    count = lax.axis_size("snp")
    traits, size = warm_start.shape
    field = ((traits, size), F32)
    table = ((traits, 128), F32)
    matrix = ((size, size), BF16)
    work = 6 * traits * size * size
    copies = (
        pltpu.VMEM((size, size), F32),
        pltpu.VMEM((traits, size), F32),
        pltpu.SemaphoreType.DMA((size // tile_of(size) + 1,)),
    )
    on_chip = [(i, i ^ 1) for i in range(count) if i ^ 1 < count]
    downward = [(i + 1, i) for i in range(1, count - 1, 2)]
    upward = [(i, i + 1) for i in range(1, count - 1, 2)]

    def shift(value, route):
        return lax.ppermute(value, "snp", route)

    def run(kernel, out, *args, **rest):
        return call(kernel, out, *args, **rest)

    hbm = pltpu.HBM
    ridge = shrinkage.reshape(1, traits)
    down = shift(warm_start, downward)
    high_n, low_n, cross = run(
        begin_odd_kernel, [matrix, matrix, field], next_block, warm_start,
        spaces={0: hbm, 1: hbm}, scratch=copies, flops=work,
    )
    high_l, low_l, own, pair = run(
        local_odd_kernel, [matrix, matrix, field, field], local_block, warm_start, cross, flops=work
    )
    up = shift(cross, upward)
    high_n, low_n, pair = run(
        begin_even_kernel, [matrix, matrix, field], next_block, warm_start, high_n, low_n, pair,
        spaces={0: hbm}, scratch=copies[::2], aliases={2: 0, 3: 1, 4: 2}, flops=work,
    )
    got_pair = shift(pair, on_chip)
    rest, high_up, low_up = run(
        prepare_odd_kernel, [field, matrix, matrix],
        own, warm_start, marginal, ridge, high_n, low_n, flops=work,
    )
    odd = functools.partial(odd_kernel, -1.0)
    odd_field, cross = run(odd, [field, field], rest, got_pair, down, high_n, low_n, high_up, low_up, ridge, flops=work)
    next_up = shift(cross, upward)
    high_l, low_l, high_up, low_up, base = run(
        prepare_even_kernel, [matrix, matrix, matrix, matrix, field],
        local_block, warm_start, marginal, ridge, got_pair, high_n, low_n,
        high_l, low_l, high_up, low_up, odd_field,
        aliases={7: 0, 8: 1, 9: 2, 10: 3}, flops=work,
    )
    join = functools.partial(join_kernel, -1.0)
    merged, pair = run(join, [field, field], base, up, odd_field, high_n, low_n, flops=work)
    up = next_up
    fields, tables = [merged], []
    odd, join = functools.partial(odd_kernel, 1.0), functools.partial(join_kernel, 1.0)
    for step in range(2, ITERS + 2):
        got_pair = shift(pair, on_chip)
        if step % 2 == 0:
            down = shift(merged, downward)
        before = fields[-2:-1]
        kernel = own_kernel if before else functools.partial(own_kernel, None)
        own, part = run(kernel, [field, table], *before, merged, high_l, low_l, flops=work)
        tables.append(part)
        if step > ITERS:
            break
        (base,) = run(pair_kernel, [field], own, got_pair, high_up, low_up, flops=work)
        if step % 2 == 0:
            (even_field,) = run(even_kernel, [field], base, up, ridge, flops=work)
            next_down = shift(even_field, downward)
            odd_field, cross = run(
                odd, [field, field],
                own, got_pair, down, high_n, low_n, high_up, low_up, even_field, flops=work,
            )
            up = shift(cross, upward)
            down = next_down
            merged, pair = run(merge_kernel, [field, field], even_field, odd_field, high_n, low_n, flops=work)
        else:
            odd_field, cross = run(
                odd, [field, field],
                own, got_pair, down, high_n, low_n, high_up, low_up, own, flops=work,
            )
            next_up = shift(cross, upward)
            merged, pair = run(join, [field, field], base, up, odd_field, high_n, low_n, flops=work)
            up = next_up
        fields.append(merged)
    lanes = -(-traits // 128) * 128
    (moments,) = run(reduce_kernel, [((count, MOMENT_ROWS, lanes), F32)], fields[-1], own, got_pair, up, *tables)
    moments = lax.all_to_all(moments, "snp", 0, 0)
    (weights,) = run(weights_kernel, [table], moments, ridge)
    return tuple(
        run(
            final_kernel, [field, field],
            weights, warm_start, *fields, own, got_pair, down, up, high_up, low_up,
            keep=False,
        )
    )


def solution(mesh):
    return jax.shard_map(
        on_device,
        mesh=mesh,
        in_specs=(
            P(("parts", "snp"), None),
            P(("parts", "snp"), None),
            P(),
            P(None, ("parts", "snp")),
            P(None, ("parts", "snp")),
        ),
        out_specs=(P(None, ("parts", "snp")), P(None, ("parts", "snp"))),
        check_vma=False,
    )
```

```python
import functools

import jax
import jax.numpy as jnp
from jax import lax
from jax.experimental import pallas as pl
from jax.experimental.pallas import tpu as pltpu
from jax.sharding import PartitionSpec as P


ITERS = 3
F32 = jnp.float32
BF16 = jnp.bfloat16
VMEM = pltpu.VMEM
MOMENT_ROWS = 8


def tile_of(size):
    return 256 if size % 256 == 0 else size


def is_odd():
    return lax.rem(lax.axis_index("snp"), 2) == 1


def halves(x):
    high = x.astype(BF16)
    return high, (x - high.astype(F32)).astype(BF16)


def dot(left, right):
    return jnp.dot(left, right, preferred_element_type=F32)


def product(both, right_high, right_low):
    rows = both.shape[0] // 2
    main = dot(both, right_high)
    return main[:rows] + main[rows:] + dot(both[:rows], right_low)


def stacked(field):
    return jnp.concatenate(halves(field), axis=0)


def coupling(both, high, low, store):
    size = high.shape[0]
    tile = tile_of(size)
    for start in range(0, size, tile):
        rows, cols = pl.ds(start, size - start), pl.ds(start, tile)
        store(start, product(both[:, start:], high[rows, cols], low[rows, cols]))


def forward(both, high, low, store):
    size = high.shape[0]
    tile = tile_of(size)
    for start in range(0, size, tile):
        rows, cols = pl.ds(0, start + tile), pl.ds(start, tile)
        store(start, product(both[:, : start + tile], high[rows, cols], low[rows, cols]))


def adding(total_ref):
    def store(start, part):
        tile = part.shape[1] - start
        if start:
            total_ref[:, pl.ds(0, start)] = total_ref[:, pl.ds(0, start)] + part[:, :start]
        total_ref[:, pl.ds(start, tile)] = part[:, start:]

    return store


def load(source_ref, parts, raw, sems):
    copies = [
        pltpu.make_async_copy(source_ref.at[part], raw.at[part], sems.at[index]) for index, part in enumerate(parts)
    ]
    for copy in copies:
        copy.start()
    return copies


def take_next(next_ref, field_ref, high_ref, low_ref, out_ref, raw, sems, field=None):
    size = raw.shape[0]
    tile = tile_of(size)
    starts = list(range(0, size, tile))
    parts = [(pl.ds(start, tile), pl.ds(0, start + tile)) for start in starts]
    if field is not None:
        ours = pltpu.make_async_copy(field_ref, field, sems.at[len(starts)])
        ours.start()
    copies = load(next_ref, parts, raw, sems)
    store = adding(out_ref)
    if field is not None:
        ours.wait()
        field_ref = field
    for start, part, copy in zip(starts, parts, copies):
        copy.wait()
        high, low = halves(raw[part])
        high_ref[part] = high
        low_ref[part] = low
        store(start, product(stacked(field_ref[:, pl.ds(start, tile)]), high, low))


def take_local(local_ref, field_ref, high_ref, low_ref, out_ref):
    size = local_ref.shape[0]
    tile = tile_of(size)
    both = stacked(field_ref[...])
    for start in range(0, size, tile):
        rows = pl.ds(start, tile)
        row = lax.broadcasted_iota(jnp.int32, (tile, size), 0) + start
        col = lax.broadcasted_iota(jnp.int32, (tile, size), 1)
        high, low = halves(local_ref[rows, :] - jnp.where(row == col, 1.0, 0.0))
        high_ref[rows, :] = high
        low_ref[rows, :] = low
        done = product(both[:, start : start + tile], high, low)
        out_ref[...] = done if start == 0 else out_ref[...] + done


def begin_odd_kernel(next_ref, start_ref, high_n, low_n, cross_ref, raw, field, sems):
    @pl.when(is_odd())
    def _():
        take_next(next_ref, start_ref, high_n, low_n, cross_ref, raw, sems, field)


def local_odd_kernel(local_ref, start_ref, after_ref, high_l, low_l, own_ref, pair_ref):
    del after_ref

    @pl.when(is_odd())
    def _():
        take_local(local_ref, start_ref, high_l, low_l, own_ref)
        pair_ref[...] = start_ref[...]


def begin_even_kernel(next_ref, start_ref, high_n_in, low_n_in, pair_in, high_n, low_n, pair_ref, raw, sems):
    del high_n_in, low_n_in, pair_in

    @pl.when(jnp.logical_not(is_odd()))
    def _():
        take_next(next_ref, start_ref, high_n, low_n, pair_ref, raw, sems)


def flip(high_in, low_in, high_ref, low_ref):
    size = high_in.shape[0]
    tile = tile_of(size)
    for row in range(0, size, tile):
        for col in range(0, row + tile, tile):
            source, target = (pl.ds(row, tile), pl.ds(col, tile)), (pl.ds(col, tile), pl.ds(row, tile))
            high_ref[target] = jnp.transpose(high_in[source])
            low_ref[target] = jnp.transpose(low_in[source])


def ridge_column(shrinkage_ref):
    traits = shrinkage_ref.shape[1]
    here = lax.broadcasted_iota(jnp.int32, (traits, traits), 0) == lax.broadcasted_iota(jnp.int32, (traits, traits), 1)
    return 1.0 + jnp.sum(jnp.where(here, shrinkage_ref[...], 0.0), axis=1, keepdims=True)


def prepare_odd_kernel(own_ref, start_ref, marginal_ref, shrinkage_ref, high_n, low_n, rest_ref, high_up, low_up):
    @pl.when(is_odd())
    def _():
        rest_ref[...] = marginal_ref[...] - ridge_column(shrinkage_ref) * start_ref[...] - own_ref[...]
        flip(high_n, low_n, high_up, low_up)


def prepare_even_kernel(
    local_ref, start_ref, marginal_ref, shrinkage_ref, got_pair_ref, high_n, low_n,
    high_l_in, low_l_in, high_up_in, low_up_in, after_ref,
    high_l, low_l, high_up, low_up, base_ref,
):
    del high_l_in, low_l_in, high_up_in, low_up_in, after_ref

    @pl.when(jnp.logical_not(is_odd()))
    def _():
        flip(high_n, low_n, high_up, low_up)
        take_local(local_ref, start_ref, high_l, low_l, base_ref)
        base_ref[...] = marginal_ref[...] - ridge_column(shrinkage_ref) * start_ref[...] - base_ref[...]
        tile = tile_of(base_ref.shape[1])

        def store(start, part):
            cols = pl.ds(start, tile)
            base_ref[:, cols] = base_ref[:, cols] - part

        forward(stacked(got_pair_ref[...]), high_up, low_up, store)


def moment(left, right):
    return jnp.sum(left * right, axis=1, keepdims=True)


def own_kernel(before_ref, field_ref, high_ref, low_ref, own_ref, moments_ref):
    field = field_ref[...]
    own_ref[...] = product(stacked(field), high_ref[...], low_ref[...])
    lane = lax.broadcasted_iota(jnp.int32, moments_ref.shape, 1)
    cross = 0.0 if before_ref is None else moment(before_ref[...], field)
    moments_ref[...] = jnp.where(lane == 0, moment(field, field), jnp.where(lane == 1, cross, 0.0))


def own_part_kernel(wanted, before_ref, field_ref, high_ref, low_ref, *refs):
    own_ref, moments_ref = refs[-2:]

    @pl.when(is_odd() if wanted else jnp.logical_not(is_odd()))
    def _():
        own_kernel(before_ref, field_ref, high_ref, low_ref, own_ref, moments_ref)


def pair_kernel(own_ref, got_pair_ref, high_up, low_up, base_ref):
    @pl.when(jnp.logical_not(is_odd()))
    def _():
        tile = tile_of(own_ref.shape[1])

        def store(start, part):
            cols = pl.ds(start, tile)
            base_ref[:, cols] = own_ref[:, cols] + part

        forward(stacked(got_pair_ref[...]), high_up, low_up, store)


def even_kernel(base_ref, got_ref, after_ref, field_ref):
    del after_ref

    @pl.when(jnp.logical_not(is_odd()))
    def _():
        field_ref[...] = base_ref[...] + got_ref[...]


def odd_kernel(sign, own_ref, got_pair_ref, got_ref, high_in, low_in, high_up, low_up, after_ref, field_ref, cross_ref):
    del after_ref

    @pl.when(is_odd())
    def _():
        tile = tile_of(own_ref.shape[1])

        def keep(start, part):
            cols = pl.ds(start, tile)
            field_ref[:, cols] = own_ref[:, cols] + sign * (got_pair_ref[:, cols] + part)

        def send(start, part):
            cross_ref[:, pl.ds(start, tile)] = part

        forward(stacked(got_ref[...]), high_up, low_up, keep)
        coupling(stacked(field_ref[...]), high_in, low_in, send)


def couple_even(field_ref, high_in, low_in, pair_ref):
    tile = tile_of(field_ref.shape[1])

    def send(start, part):
        pair_ref[:, pl.ds(start, tile)] = part

    coupling(stacked(field_ref[...]), high_in, low_in, send)


def couple_kernel(field_ref, high_in, low_in, pair_ref):
    @pl.when(jnp.logical_not(is_odd()))
    def _():
        couple_even(field_ref, high_in, low_in, pair_ref)


def merge_kernel(even_ref, odd_ref, field_ref):
    @pl.when(is_odd())
    def _():
        field_ref[...] = odd_ref[...]

    @pl.when(jnp.logical_not(is_odd()))
    def _():
        field_ref[...] = even_ref[...]


def join_kernel(sign, base_ref, got_ref, odd_ref, high_in, low_in, field_ref, pair_ref):
    @pl.when(is_odd())
    def _():
        field_ref[...] = odd_ref[...]
        pair_ref[...] = odd_ref[...]

    @pl.when(jnp.logical_not(is_odd()))
    def _():
        field_ref[...] = base_ref[...] + sign * got_ref[...]
        couple_even(field_ref, high_in, low_in, pair_ref)


def reduce_kernel(field_ref, own_ref, got_pair_ref, got_up_ref, one_ref, two_ref, three_ref, out_ref):
    traits = field_ref.shape[0]
    lower = jnp.where(is_odd(), got_pair_ref[...], got_up_ref[...])
    last = moment(field_ref[...], own_ref[...] + 2.0 * lower)
    lane = lax.broadcasted_iota(jnp.int32, (traits, 128), 1)
    parts = (
        one_ref[:, 0:1],
        two_ref[:, 1:2],
        two_ref[:, 0:1],
        three_ref[:, 1:2],
        three_ref[:, 0:1],
        last,
    )
    table = jnp.zeros((traits, 128), F32)
    for index, part in enumerate(parts):
        table = jnp.where(lane == index, part, table)
    lanes = out_ref.shape[2]
    if lanes > traits:
        table = jnp.concatenate([table, jnp.zeros((lanes - traits, 128), F32)], axis=0)
    rows = jnp.transpose(table)[:MOMENT_ROWS]
    for index in range(out_ref.shape[0]):
        out_ref[index] = rows


def coefficients(moments, shift):
    def inner(left, right):
        total = None
        for i, a in enumerate(left):
            for j, b in enumerate(right):
                term = (a * b) * moments[i + j]
                total = term if total is None else total + term
        return total

    one = jnp.ones_like(shift)
    zero = jnp.zeros_like(shift)
    residual, direction, gain = [one], [one], []
    norm_now = moments[0]
    for step in range(ITERS):
        image = [shift * a + b for a, b in zip(direction + [zero], [zero] + direction)]
        alpha = norm_now / inner(direction, image)
        gain = [a + alpha * b for a, b in zip(gain + [zero], direction)]
        residual = [a - alpha * b for a, b in zip(residual + [zero], image)]
        if step + 1 < ITERS:
            norm_next = inner(residual, residual)
            ratio = norm_next / norm_now
            direction = [a + ratio * b for a, b in zip(residual, direction + [zero])]
            norm_now = norm_next
    return gain, residual


def weights_kernel(table_ref, shrinkage_ref, weights_ref):
    sums = jnp.sum(table_ref[...], axis=0)
    traits, lanes = weights_ref.shape[0], sums.shape[1]
    shift = 1.0 + shrinkage_ref[...]
    moments = [sums[i : i + 1, :traits] for i in range(2 * ITERS)]
    gain, residual = coefficients(moments, shift)
    row = lax.broadcasted_iota(jnp.int32, (lanes, traits), 0)
    table = jnp.zeros((lanes, traits), F32)
    for index, part in enumerate(gain + residual):
        table = jnp.where(row == index, part, table)
    weights_ref[...] = jnp.transpose(table)


def final_kernel(
    weights_ref, start_ref, zero_ref, one_ref, two_ref, own_ref, got_pair_ref, got_down_ref, got_up_ref,
    high_up, low_up, solution_ref, residual_ref,
):
    tile = tile_of(own_ref.shape[1])
    weights = [weights_ref[:, i : i + 1] for i in range(2 * ITERS + 1)]
    gain, residual = weights[:ITERS], weights[ITERS:]
    odd = is_odd()
    upper = jnp.where(odd, got_down_ref[...], got_pair_ref[...])
    lower = jnp.where(odd, got_pair_ref[...], got_up_ref[...])
    zero, one, two = zero_ref[...], one_ref[...], two_ref[...]
    solution_ref[...] = start_ref[...] + gain[0] * zero + gain[1] * one + gain[2] * two
    base = residual[0] * zero + residual[1] * one + residual[2] * two + residual[3] * (own_ref[...] + lower)

    def store(start, part):
        residual_ref[:, pl.ds(start, tile)] = base[:, start : start + tile] + residual[3] * part

    forward(stacked(upper), high_up, low_up, store)


def call(kernel, out, *args, spaces=None, scratch=(), limit=12, aliases=None, keep=True, flops=0):
    spaces = spaces or {}
    places = [spaces.get(i, VMEM) for i in range(len(args))]
    args = [
        arg if place is pltpu.SMEM else pltpu.with_memory_space_constraint(arg, place)
        for arg, place in zip(args, places)
    ]
    make = VMEM if keep else jax.ShapeDtypeStruct
    return pl.pallas_call(
        kernel,
        out_shape=[make(shape, dtype) for shape, dtype in out],
        in_specs=[pl.BlockSpec(memory_space=place) for place in places],
        out_specs=[pl.BlockSpec(memory_space=VMEM) for _ in out],
        scratch_shapes=scratch,
        input_output_aliases=aliases or {},
        cost_estimate=pl.CostEstimate(flops=flops, bytes_accessed=0, transcendentals=0) if flops else None,
        compiler_params=pltpu.CompilerParams(vmem_limit_bytes=limit * 1024 * 1024),
    )(*args)


def on_device(local_block, next_block, shrinkage, marginal, warm_start):
    count = lax.axis_size("snp")
    traits, size = warm_start.shape
    field = ((traits, size), F32)
    table = ((traits, 128), F32)
    matrix = ((size, size), BF16)
    work = 6 * traits * size * size
    copies = (
        pltpu.VMEM((size, size), F32),
        pltpu.VMEM((traits, size), F32),
        pltpu.SemaphoreType.DMA((size // tile_of(size) + 1,)),
    )
    on_chip = [(i, i ^ 1) for i in range(count) if i ^ 1 < count]
    downward = [(i + 1, i) for i in range(1, count - 1, 2)]
    upward = [(i, i + 1) for i in range(1, count - 1, 2)]

    def shift(value, route):
        return lax.ppermute(value, "snp", route)

    def run(kernel, out, *args, **rest):
        return call(kernel, out, *args, **rest)

    hbm = pltpu.HBM
    ridge = shrinkage.reshape(1, traits)
    down = shift(warm_start, downward)
    high_n, low_n, cross = run(
        begin_odd_kernel, [matrix, matrix, field], next_block, warm_start,
        spaces={0: hbm, 1: hbm}, scratch=copies, flops=work,
    )
    high_l, low_l, own, pair = run(
        local_odd_kernel, [matrix, matrix, field, field], local_block, warm_start, cross, flops=work
    )
    up = shift(cross, upward)
    high_n, low_n, pair = run(
        begin_even_kernel, [matrix, matrix, field], next_block, warm_start, high_n, low_n, pair,
        spaces={0: hbm}, scratch=copies[::2], aliases={2: 0, 3: 1, 4: 2}, flops=work,
    )
    got_pair = shift(pair, on_chip)
    rest, high_up, low_up = run(
        prepare_odd_kernel, [field, matrix, matrix],
        own, warm_start, marginal, ridge, high_n, low_n, flops=work,
    )
    odd = functools.partial(odd_kernel, -1.0)
    odd_field, cross = run(odd, [field, field], rest, got_pair, down, high_n, low_n, high_up, low_up, ridge, flops=work)
    next_up = shift(cross, upward)
    high_l, low_l, high_up, low_up, base = run(
        prepare_even_kernel, [matrix, matrix, matrix, matrix, field],
        local_block, warm_start, marginal, ridge, got_pair, high_n, low_n,
        high_l, low_l, high_up, low_up, odd_field,
        aliases={7: 0, 8: 1, 9: 2, 10: 3}, flops=work,
    )
    join = functools.partial(join_kernel, -1.0)
    merged, pair = run(join, [field, field], base, up, odd_field, high_n, low_n, flops=work)
    up = next_up
    fields, tables = [merged], []
    odd, join = functools.partial(odd_kernel, 1.0), functools.partial(join_kernel, 1.0)
    for step in range(2, ITERS + 2):
        got_pair = shift(pair, on_chip)
        if step % 2 == 0:
            down = shift(merged, downward)
        before = fields[-2:-1]
        kernel = own_kernel if before else functools.partial(own_kernel, None)
        if step == 3:
            inputs = (*before, merged, high_l, low_l)
            own, part = run(functools.partial(own_part_kernel, False), [field, table], *inputs, flops=work)
            own, part = run(
                functools.partial(own_part_kernel, True), [field, table], *inputs, own, part,
                aliases={4: 0, 5: 1}, flops=work,
            )
        else:
            own, part = run(kernel, [field, table], *before, merged, high_l, low_l, flops=work)
        tables.append(part)
        if step > ITERS:
            break
        (base,) = run(pair_kernel, [field], own, got_pair, high_up, low_up, flops=work)
        if step % 2 == 0:
            (even_field,) = run(even_kernel, [field], base, up, ridge, flops=work)
            next_down = shift(even_field, downward)
            (early,) = run(couple_kernel, [field], even_field, high_n, low_n, flops=work)
            got_early = shift(early, on_chip)
            odd_field, cross = run(
                odd, [field, field],
                own, got_pair, down, high_n, low_n, high_up, low_up, even_field, flops=work,
            )
            up = shift(cross, upward)
            down = next_down
            (merged,) = run(merge_kernel, [field], even_field, odd_field, flops=work)
            pair = merged
        else:
            odd_field, cross = run(
                odd, [field, field],
                own, got_early, down, high_n, low_n, high_up, low_up, own, flops=work,
            )
            next_up = shift(cross, upward)
            merged, pair = run(join, [field, field], base, up, odd_field, high_n, low_n, flops=work)
            up = next_up
        fields.append(merged)
    lanes = -(-traits // 128) * 128
    (moments,) = run(reduce_kernel, [((count, MOMENT_ROWS, lanes), F32)], fields[-1], own, got_pair, up, *tables)
    moments = lax.all_to_all(moments, "snp", 0, 0)
    (weights,) = run(weights_kernel, [table], moments, ridge)
    return tuple(
        run(
            final_kernel, [field, field],
            weights, warm_start, *fields, own, got_pair, down, up, high_up, low_up,
            keep=False,
        )
    )


def solution(mesh):
    return jax.shard_map(
        on_device,
        mesh=mesh,
        in_specs=(
            P(("parts", "snp"), None),
            P(("parts", "snp"), None),
            P(),
            P(None, ("parts", "snp")),
            P(None, ("parts", "snp")),
        ),
        out_specs=(P(None, ("parts", "snp")), P(None, ("parts", "snp"))),
        check_vma=False,
    )
```

```python
import functools

import jax
import jax.numpy as jnp
from jax import lax
from jax.experimental import pallas as pl
from jax.experimental.pallas import tpu as pltpu
from jax.sharding import PartitionSpec as P


ITERS = 3
F32 = jnp.float32
BF16 = jnp.bfloat16
VMEM = pltpu.VMEM
MOMENT_ROWS = 8


def tile_of(size):
    return 256 if size % 256 == 0 else size


def is_odd():
    return lax.rem(lax.axis_index("snp"), 2) == 1


def halves(x):
    high = x.astype(BF16)
    return high, (x - high.astype(F32)).astype(BF16)


def dot(left, right):
    return jnp.dot(left, right, preferred_element_type=F32)


def product(both, right_high, right_low):
    rows = both.shape[0] // 2
    main = dot(both, right_high)
    return main[:rows] + main[rows:] + dot(both[:rows], right_low)


def stacked(field):
    return jnp.concatenate(halves(field), axis=0)


def coupling(both, high, low, store):
    size = high.shape[0]
    tile = tile_of(size)
    for start in range(0, size, tile):
        rows, cols = pl.ds(start, size - start), pl.ds(start, tile)
        store(start, product(both[:, start:], high[rows, cols], low[rows, cols]))


def forward(both, high, low, store):
    size = high.shape[0]
    tile = tile_of(size)
    for start in range(0, size, tile):
        rows, cols = pl.ds(0, start + tile), pl.ds(start, tile)
        store(start, product(both[:, : start + tile], high[rows, cols], low[rows, cols]))


def adding(total_ref):
    def store(start, part):
        tile = part.shape[1] - start
        if start:
            total_ref[:, pl.ds(0, start)] = total_ref[:, pl.ds(0, start)] + part[:, :start]
        total_ref[:, pl.ds(start, tile)] = part[:, start:]

    return store


def load(source_ref, parts, raw, sems):
    copies = [
        pltpu.make_async_copy(source_ref.at[part], raw.at[part], sems.at[index]) for index, part in enumerate(parts)
    ]
    for copy in copies:
        copy.start()
    return copies


def take_next(next_ref, field_ref, high_ref, low_ref, out_ref, raw, sems, field=None):
    size = raw.shape[0]
    tile = tile_of(size)
    starts = list(range(0, size, tile))
    parts = [(pl.ds(start, tile), pl.ds(0, start + tile)) for start in starts]
    if field is not None:
        ours = pltpu.make_async_copy(field_ref, field, sems.at[len(starts)])
        ours.start()
    copies = load(next_ref, parts, raw, sems)
    store = adding(out_ref)
    if field is not None:
        ours.wait()
        field_ref = field
    for start, part, copy in zip(starts, parts, copies):
        copy.wait()
        high, low = halves(raw[part])
        high_ref[part] = high
        low_ref[part] = low
        store(start, product(stacked(field_ref[:, pl.ds(start, tile)]), high, low))


def take_local(local_ref, field_ref, high_ref, low_ref, out_ref):
    size = local_ref.shape[0]
    tile = tile_of(size)
    both = stacked(field_ref[...])
    for start in range(0, size, tile):
        rows = pl.ds(start, tile)
        row = lax.broadcasted_iota(jnp.int32, (tile, size), 0) + start
        col = lax.broadcasted_iota(jnp.int32, (tile, size), 1)
        high, low = halves(local_ref[rows, :] - jnp.where(row == col, 1.0, 0.0))
        high_ref[rows, :] = high
        low_ref[rows, :] = low
        done = product(both[:, start : start + tile], high, low)
        out_ref[...] = done if start == 0 else out_ref[...] + done


def begin_odd_kernel(next_ref, start_ref, high_n, low_n, cross_ref, raw, field, sems):
    @pl.when(is_odd())
    def _():
        take_next(next_ref, start_ref, high_n, low_n, cross_ref, raw, sems, field)


def local_odd_kernel(local_ref, start_ref, after_ref, high_l, low_l, own_ref, pair_ref):
    del after_ref

    @pl.when(is_odd())
    def _():
        take_local(local_ref, start_ref, high_l, low_l, own_ref)
        pair_ref[...] = start_ref[...]


def begin_even_kernel(next_ref, start_ref, high_n_in, low_n_in, pair_in, high_n, low_n, pair_ref, raw, sems):
    del high_n_in, low_n_in, pair_in

    @pl.when(jnp.logical_not(is_odd()))
    def _():
        take_next(next_ref, start_ref, high_n, low_n, pair_ref, raw, sems)


def flip(high_in, low_in, high_ref, low_ref):
    size = high_in.shape[0]
    tile = tile_of(size)
    for row in range(0, size, tile):
        for col in range(0, row + tile, tile):
            source, target = (pl.ds(row, tile), pl.ds(col, tile)), (pl.ds(col, tile), pl.ds(row, tile))
            high_ref[target] = jnp.transpose(high_in[source])
            low_ref[target] = jnp.transpose(low_in[source])


def ridge_column(shrinkage_ref):
    traits = shrinkage_ref.shape[1]
    here = lax.broadcasted_iota(jnp.int32, (traits, traits), 0) == lax.broadcasted_iota(jnp.int32, (traits, traits), 1)
    return 1.0 + jnp.sum(jnp.where(here, shrinkage_ref[...], 0.0), axis=1, keepdims=True)


def prepare_odd_kernel(own_ref, start_ref, marginal_ref, shrinkage_ref, high_n, low_n, rest_ref, high_up, low_up):
    @pl.when(is_odd())
    def _():
        rest_ref[...] = marginal_ref[...] - ridge_column(shrinkage_ref) * start_ref[...] - own_ref[...]
        flip(high_n, low_n, high_up, low_up)


def prepare_even_kernel(
    local_ref, start_ref, marginal_ref, shrinkage_ref, got_pair_ref, high_n, low_n,
    high_l_in, low_l_in, high_up_in, low_up_in, after_ref,
    high_l, low_l, high_up, low_up, base_ref,
):
    del high_l_in, low_l_in, high_up_in, low_up_in, after_ref

    @pl.when(jnp.logical_not(is_odd()))
    def _():
        flip(high_n, low_n, high_up, low_up)
        take_local(local_ref, start_ref, high_l, low_l, base_ref)
        base_ref[...] = marginal_ref[...] - ridge_column(shrinkage_ref) * start_ref[...] - base_ref[...]
        tile = tile_of(base_ref.shape[1])

        def store(start, part):
            cols = pl.ds(start, tile)
            base_ref[:, cols] = base_ref[:, cols] - part

        forward(stacked(got_pair_ref[...]), high_up, low_up, store)


def moment(left, right):
    return jnp.sum(left * right, axis=1, keepdims=True)


def own_kernel(before_ref, field_ref, high_ref, low_ref, own_ref, moments_ref):
    field = field_ref[...]
    own_ref[...] = product(stacked(field), high_ref[...], low_ref[...])
    lane = lax.broadcasted_iota(jnp.int32, moments_ref.shape, 1)
    cross = 0.0 if before_ref is None else moment(before_ref[...], field)
    moments_ref[...] = jnp.where(lane == 0, moment(field, field), jnp.where(lane == 1, cross, 0.0))


def own_part_kernel(wanted, before_ref, field_ref, high_ref, low_ref, *refs):
    own_ref, moments_ref = refs[-2:]

    @pl.when(is_odd() if wanted else jnp.logical_not(is_odd()))
    def _():
        own_kernel(before_ref, field_ref, high_ref, low_ref, own_ref, moments_ref)


def pair_kernel(own_ref, got_pair_ref, high_up, low_up, base_ref):
    @pl.when(jnp.logical_not(is_odd()))
    def _():
        tile = tile_of(own_ref.shape[1])

        def store(start, part):
            cols = pl.ds(start, tile)
            base_ref[:, cols] = own_ref[:, cols] + part

        forward(stacked(got_pair_ref[...]), high_up, low_up, store)


def even_kernel(base_ref, got_ref, after_ref, field_ref):
    del after_ref

    @pl.when(jnp.logical_not(is_odd()))
    def _():
        field_ref[...] = base_ref[...] + got_ref[...]


def odd_kernel(sign, own_ref, got_pair_ref, got_ref, high_in, low_in, high_up, low_up, after_ref, field_ref, cross_ref):
    del after_ref

    @pl.when(is_odd())
    def _():
        tile = tile_of(own_ref.shape[1])

        def keep(start, part):
            cols = pl.ds(start, tile)
            field_ref[:, cols] = own_ref[:, cols] + sign * (got_pair_ref[:, cols] + part)

        def send(start, part):
            cross_ref[:, pl.ds(start, tile)] = part

        forward(stacked(got_ref[...]), high_up, low_up, keep)
        coupling(stacked(field_ref[...]), high_in, low_in, send)


def couple_even(field_ref, high_in, low_in, pair_ref):
    tile = tile_of(field_ref.shape[1])

    def send(start, part):
        pair_ref[:, pl.ds(start, tile)] = part

    coupling(stacked(field_ref[...]), high_in, low_in, send)


def couple_kernel(field_ref, high_in, low_in, pair_ref):
    @pl.when(jnp.logical_not(is_odd()))
    def _():
        couple_even(field_ref, high_in, low_in, pair_ref)


def merge_kernel(even_ref, odd_ref, field_ref):
    @pl.when(is_odd())
    def _():
        field_ref[...] = odd_ref[...]

    @pl.when(jnp.logical_not(is_odd()))
    def _():
        field_ref[...] = even_ref[...]


def join_kernel(sign, base_ref, got_ref, odd_ref, high_in, low_in, field_ref, pair_ref):
    @pl.when(is_odd())
    def _():
        field_ref[...] = odd_ref[...]
        pair_ref[...] = odd_ref[...]

    @pl.when(jnp.logical_not(is_odd()))
    def _():
        field_ref[...] = base_ref[...] + sign * got_ref[...]
        couple_even(field_ref, high_in, low_in, pair_ref)


def reduce_kernel(field_ref, own_ref, got_pair_ref, got_up_ref, one_ref, two_ref, three_ref, out_ref):
    traits = field_ref.shape[0]
    lower = jnp.where(is_odd(), got_pair_ref[...], got_up_ref[...])
    last = moment(field_ref[...], own_ref[...] + 2.0 * lower)
    lane = lax.broadcasted_iota(jnp.int32, (traits, 128), 1)
    parts = (
        one_ref[:, 0:1],
        two_ref[:, 1:2],
        two_ref[:, 0:1],
        three_ref[:, 1:2],
        three_ref[:, 0:1],
        last,
    )
    table = jnp.zeros((traits, 128), F32)
    for index, part in enumerate(parts):
        table = jnp.where(lane == index, part, table)
    lanes = out_ref.shape[2]
    if lanes > traits:
        table = jnp.concatenate([table, jnp.zeros((lanes - traits, 128), F32)], axis=0)
    rows = jnp.transpose(table)[:MOMENT_ROWS]
    for index in range(out_ref.shape[0]):
        out_ref[index] = rows


def coefficients(moments, shift):
    def inner(left, right):
        total = None
        for i, a in enumerate(left):
            for j, b in enumerate(right):
                term = (a * b) * moments[i + j]
                total = term if total is None else total + term
        return total

    one = jnp.ones_like(shift)
    zero = jnp.zeros_like(shift)
    residual, direction, gain = [one], [one], []
    norm_now = moments[0]
    for step in range(ITERS):
        image = [shift * a + b for a, b in zip(direction + [zero], [zero] + direction)]
        alpha = norm_now / inner(direction, image)
        gain = [a + alpha * b for a, b in zip(gain + [zero], direction)]
        residual = [a - alpha * b for a, b in zip(residual + [zero], image)]
        if step + 1 < ITERS:
            norm_next = inner(residual, residual)
            ratio = norm_next / norm_now
            direction = [a + ratio * b for a, b in zip(residual, direction + [zero])]
            norm_now = norm_next
    return gain, residual


def weights_kernel(table_ref, shrinkage_ref, weights_ref):
    sums = jnp.sum(table_ref[...], axis=0)
    traits, lanes = weights_ref.shape[0], sums.shape[1]
    shift = 1.0 + shrinkage_ref[...]
    moments = [sums[i : i + 1, :traits] for i in range(2 * ITERS)]
    gain, residual = coefficients(moments, shift)
    row = lax.broadcasted_iota(jnp.int32, (lanes, traits), 0)
    table = jnp.zeros((lanes, traits), F32)
    for index, part in enumerate(gain + residual):
        table = jnp.where(row == index, part, table)
    weights_ref[...] = jnp.transpose(table)


def final_kernel(
    weights_ref, start_ref, zero_ref, one_ref, two_ref, own_ref, got_pair_ref, got_down_ref, got_up_ref,
    high_up, low_up, solution_ref, residual_ref,
):
    tile = tile_of(own_ref.shape[1])
    weights = [weights_ref[:, i : i + 1] for i in range(2 * ITERS + 1)]
    gain, residual = weights[:ITERS], weights[ITERS:]
    odd = is_odd()
    upper = jnp.where(odd, got_down_ref[...], got_pair_ref[...])
    lower = jnp.where(odd, got_pair_ref[...], got_up_ref[...])
    zero, one, two = zero_ref[...], one_ref[...], two_ref[...]
    solution_ref[...] = start_ref[...] + gain[0] * zero + gain[1] * one + gain[2] * two
    base = residual[0] * zero + residual[1] * one + residual[2] * two + residual[3] * (own_ref[...] + lower)

    def store(start, part):
        residual_ref[:, pl.ds(start, tile)] = base[:, start : start + tile] + residual[3] * part

    forward(stacked(upper), high_up, low_up, store)


def call(kernel, out, *args, spaces=None, scratch=(), limit=12, aliases=None, keep=True, flops=0):
    spaces = spaces or {}
    places = [spaces.get(i, VMEM) for i in range(len(args))]
    args = [
        arg if place is pltpu.SMEM else pltpu.with_memory_space_constraint(arg, place)
        for arg, place in zip(args, places)
    ]
    make = VMEM if keep else jax.ShapeDtypeStruct
    return pl.pallas_call(
        kernel,
        out_shape=[make(shape, dtype) for shape, dtype in out],
        in_specs=[pl.BlockSpec(memory_space=place) for place in places],
        out_specs=[pl.BlockSpec(memory_space=VMEM) for _ in out],
        scratch_shapes=scratch,
        input_output_aliases=aliases or {},
        cost_estimate=pl.CostEstimate(flops=flops, bytes_accessed=0, transcendentals=0) if flops else None,
        compiler_params=pltpu.CompilerParams(vmem_limit_bytes=limit * 1024 * 1024),
    )(*args)


def on_device(local_block, next_block, shrinkage, marginal, warm_start):
    count = lax.axis_size("snp")
    traits, size = warm_start.shape
    field = ((traits, size), F32)
    table = ((traits, 128), F32)
    matrix = ((size, size), BF16)
    work = 6 * traits * size * size
    copies = (
        pltpu.VMEM((size, size), F32),
        pltpu.VMEM((traits, size), F32),
        pltpu.SemaphoreType.DMA((size // tile_of(size) + 1,)),
    )
    on_chip = [(i, i ^ 1) for i in range(count) if i ^ 1 < count]
    downward = [(i + 1, i) for i in range(1, count - 1, 2)]
    upward = [(i, i + 1) for i in range(1, count - 1, 2)]

    def shift(value, route):
        return lax.ppermute(value, "snp", route)

    def run(kernel, out, *args, **rest):
        return call(kernel, out, *args, **rest)

    hbm = pltpu.HBM
    ridge = shrinkage.reshape(1, traits)
    down = shift(warm_start, downward)
    high_n, low_n, cross = run(
        begin_odd_kernel, [matrix, matrix, field], next_block, warm_start,
        spaces={0: hbm, 1: hbm}, scratch=copies, flops=work,
    )
    high_l, low_l, own, pair = run(
        local_odd_kernel, [matrix, matrix, field, field], local_block, warm_start, cross, flops=work
    )
    up = shift(cross, upward)
    high_n, low_n, pair = run(
        begin_even_kernel, [matrix, matrix, field], next_block, warm_start, high_n, low_n, pair,
        spaces={0: hbm}, scratch=copies[::2], aliases={2: 0, 3: 1, 4: 2}, flops=work,
    )
    got_pair = shift(pair, on_chip)
    rest, high_up, low_up = run(
        prepare_odd_kernel, [field, matrix, matrix],
        own, warm_start, marginal, ridge, high_n, low_n, flops=work,
    )
    odd = functools.partial(odd_kernel, -1.0)
    odd_field, cross = run(odd, [field, field], rest, got_pair, down, high_n, low_n, high_up, low_up, ridge, flops=work)
    next_up = shift(cross, upward)
    high_l, low_l, high_up, low_up, base = run(
        prepare_even_kernel, [matrix, matrix, matrix, matrix, field],
        local_block, warm_start, marginal, ridge, got_pair, high_n, low_n,
        high_l, low_l, high_up, low_up, odd_field,
        aliases={7: 0, 8: 1, 9: 2, 10: 3}, flops=work,
    )
    join = functools.partial(join_kernel, -1.0)
    got_early = shift(odd_field, on_chip)
    merged, pair = run(join, [field, field], base, up, odd_field, high_n, low_n, flops=work)
    up = next_up
    fields, tables = [merged], []
    odd, join = functools.partial(odd_kernel, 1.0), functools.partial(join_kernel, 1.0)
    for step in range(2, ITERS + 2):
        got_pair = shift(pair, on_chip)
        if step % 2 == 0:
            down = shift(merged, downward)
        before = fields[-2:-1]
        kernel = own_kernel if before else functools.partial(own_kernel, None)
        if step < 4:
            split = functools.partial
            kernels = [split(own_part_kernel, odd_part, *(() if before else (None,))) for odd_part in (False, True)]
            inputs = (*before, merged, high_l, low_l)
            own, part = run(kernels[0], [field, table], *inputs, flops=work)
            own, part = run(
                kernels[1], [field, table], *inputs, own, part,
                aliases={len(inputs): 0, len(inputs) + 1: 1}, flops=work,
            )
        else:
            own, part = run(kernel, [field, table], *before, merged, high_l, low_l, flops=work)
        tables.append(part)
        if step > ITERS:
            break
        there = got_early if step == 2 else got_pair
        (base,) = run(pair_kernel, [field], own, there, high_up, low_up, flops=work)
        if step % 2 == 0:
            (even_field,) = run(even_kernel, [field], base, up, ridge, flops=work)
            next_down = shift(even_field, downward)
            (early,) = run(couple_kernel, [field], even_field, high_n, low_n, flops=work)
            got_early = shift(early, on_chip)
            odd_field, cross = run(
                odd, [field, field],
                own, got_pair, down, high_n, low_n, high_up, low_up, even_field, flops=work,
            )
            up = shift(cross, upward)
            down = next_down
            (merged,) = run(merge_kernel, [field], even_field, odd_field, flops=work)
            pair = merged
        else:
            odd_field, cross = run(
                odd, [field, field],
                own, got_early, down, high_n, low_n, high_up, low_up, own, flops=work,
            )
            next_up = shift(cross, upward)
            merged, pair = run(join, [field, field], base, up, odd_field, high_n, low_n, flops=work)
            up = next_up
        fields.append(merged)
    lanes = -(-traits // 128) * 128
    (moments,) = run(reduce_kernel, [((count, MOMENT_ROWS, lanes), F32)], fields[-1], own, got_pair, up, *tables)
    moments = lax.all_to_all(moments, "snp", 0, 0)
    (weights,) = run(weights_kernel, [table], moments, ridge)
    return tuple(
        run(
            final_kernel, [field, field],
            weights, warm_start, *fields, own, got_pair, down, up, high_up, low_up,
            keep=False,
        )
    )


def solution(mesh):
    return jax.shard_map(
        on_device,
        mesh=mesh,
        in_specs=(
            P(("parts", "snp"), None),
            P(("parts", "snp"), None),
            P(),
            P(None, ("parts", "snp")),
            P(None, ("parts", "snp")),
        ),
        out_specs=(P(None, ("parts", "snp")), P(None, ("parts", "snp"))),
        check_vma=False,
    )
```

```python
import functools

import jax
import jax.numpy as jnp
from jax import lax
from jax.experimental import pallas as pl
from jax.experimental.pallas import tpu as pltpu
from jax.sharding import PartitionSpec as P


ITERS = 3
F32 = jnp.float32
BF16 = jnp.bfloat16
VMEM = pltpu.VMEM
MOMENT_ROWS = 8


def tile_of(size):
    return 256 if size % 256 == 0 else size


def is_odd():
    return lax.rem(lax.axis_index("snp"), 2) == 1


def halves(x):
    high = x.astype(BF16)
    return high, (x - high.astype(F32)).astype(BF16)


def dot(left, right):
    return jnp.dot(left, right, preferred_element_type=F32)


def product(both, right_high, right_low):
    rows = both.shape[0] // 2
    main = dot(both, right_high)
    return main[:rows] + main[rows:] + dot(both[:rows], right_low)


def stacked(field):
    return jnp.concatenate(halves(field), axis=0)


def coupling(both, high, low, store):
    size = high.shape[0]
    tile = tile_of(size)
    for start in range(0, size, tile):
        rows, cols = pl.ds(start, size - start), pl.ds(start, tile)
        store(start, product(both[:, start:], high[rows, cols], low[rows, cols]))


def forward(both, high, low, store):
    size = high.shape[0]
    tile = tile_of(size)
    for start in range(0, size, tile):
        rows, cols = pl.ds(0, start + tile), pl.ds(start, tile)
        store(start, product(both[:, : start + tile], high[rows, cols], low[rows, cols]))


def adding(total_ref):
    def store(start, part):
        tile = part.shape[1] - start
        if start:
            total_ref[:, pl.ds(0, start)] = total_ref[:, pl.ds(0, start)] + part[:, :start]
        total_ref[:, pl.ds(start, tile)] = part[:, start:]

    return store


def load(source_ref, parts, raw, sems):
    copies = [
        pltpu.make_async_copy(source_ref.at[part], raw.at[part], sems.at[index]) for index, part in enumerate(parts)
    ]
    for copy in copies:
        copy.start()
    return copies


def take_next(next_ref, field_ref, high_ref, low_ref, out_ref, raw, sems, field=None):
    size = raw.shape[0]
    tile = tile_of(size)
    starts = list(range(0, size, tile))
    parts = [(pl.ds(start, tile), pl.ds(0, start + tile)) for start in starts]
    if field is not None:
        ours = pltpu.make_async_copy(field_ref, field, sems.at[len(starts)])
        ours.start()
    copies = load(next_ref, parts, raw, sems)
    store = adding(out_ref)
    if field is not None:
        ours.wait()
        field_ref = field
    for start, part, copy in zip(starts, parts, copies):
        copy.wait()
        high, low = halves(raw[part])
        high_ref[part] = high
        low_ref[part] = low
        store(start, product(stacked(field_ref[:, pl.ds(start, tile)]), high, low))


def take_local(local_ref, field_ref, high_ref, low_ref, out_ref):
    size = local_ref.shape[0]
    tile = tile_of(size)
    both = stacked(field_ref[...])
    for start in range(0, size, tile):
        rows = pl.ds(start, tile)
        row = lax.broadcasted_iota(jnp.int32, (tile, size), 0) + start
        col = lax.broadcasted_iota(jnp.int32, (tile, size), 1)
        high, low = halves(local_ref[rows, :] - jnp.where(row == col, 1.0, 0.0))
        high_ref[rows, :] = high
        low_ref[rows, :] = low
        done = product(both[:, start : start + tile], high, low)
        out_ref[...] = done if start == 0 else out_ref[...] + done


def begin_odd_kernel(next_ref, start_ref, high_n, low_n, cross_ref, raw, field, sems):
    @pl.when(is_odd())
    def _():
        take_next(next_ref, start_ref, high_n, low_n, cross_ref, raw, sems, field)


def local_odd_kernel(local_ref, start_ref, after_ref, high_l, low_l, own_ref, pair_ref):
    del after_ref

    @pl.when(is_odd())
    def _():
        take_local(local_ref, start_ref, high_l, low_l, own_ref)
        pair_ref[...] = start_ref[...]


def begin_even_kernel(next_ref, start_ref, high_n_in, low_n_in, pair_in, high_n, low_n, pair_ref, raw, sems):
    del high_n_in, low_n_in, pair_in

    @pl.when(jnp.logical_not(is_odd()))
    def _():
        take_next(next_ref, start_ref, high_n, low_n, pair_ref, raw, sems)


def flip(high_in, low_in, high_ref, low_ref):
    size = high_in.shape[0]
    tile = tile_of(size)
    for row in range(0, size, tile):
        for col in range(0, row + tile, tile):
            source, target = (pl.ds(row, tile), pl.ds(col, tile)), (pl.ds(col, tile), pl.ds(row, tile))
            high_ref[target] = jnp.transpose(high_in[source])
            low_ref[target] = jnp.transpose(low_in[source])


def ridge_column(shrinkage_ref):
    traits = shrinkage_ref.shape[1]
    here = lax.broadcasted_iota(jnp.int32, (traits, traits), 0) == lax.broadcasted_iota(jnp.int32, (traits, traits), 1)
    return 1.0 + jnp.sum(jnp.where(here, shrinkage_ref[...], 0.0), axis=1, keepdims=True)


def prepare_odd_kernel(own_ref, start_ref, marginal_ref, shrinkage_ref, high_n, low_n, rest_ref, high_up, low_up):
    @pl.when(is_odd())
    def _():
        rest_ref[...] = marginal_ref[...] - ridge_column(shrinkage_ref) * start_ref[...] - own_ref[...]
        flip(high_n, low_n, high_up, low_up)


def prepare_even_kernel(
    local_ref, start_ref, marginal_ref, shrinkage_ref, got_pair_ref, high_n, low_n,
    high_l_in, low_l_in, high_up_in, low_up_in, after_ref,
    high_l, low_l, high_up, low_up, base_ref,
):
    del high_l_in, low_l_in, high_up_in, low_up_in, after_ref

    @pl.when(jnp.logical_not(is_odd()))
    def _():
        flip(high_n, low_n, high_up, low_up)
        take_local(local_ref, start_ref, high_l, low_l, base_ref)
        base_ref[...] = marginal_ref[...] - ridge_column(shrinkage_ref) * start_ref[...] - base_ref[...]
        tile = tile_of(base_ref.shape[1])

        def store(start, part):
            cols = pl.ds(start, tile)
            base_ref[:, cols] = base_ref[:, cols] - part

        forward(stacked(got_pair_ref[...]), high_up, low_up, store)


def moment(left, right):
    return jnp.sum(left * right, axis=1, keepdims=True)


def own_kernel(before_ref, field_ref, high_ref, low_ref, own_ref, moments_ref):
    field = field_ref[...]
    own_ref[...] = product(stacked(field), high_ref[...], low_ref[...])
    lane = lax.broadcasted_iota(jnp.int32, moments_ref.shape, 1)
    cross = 0.0 if before_ref is None else moment(before_ref[...], field)
    moments_ref[...] = jnp.where(lane == 0, moment(field, field), jnp.where(lane == 1, cross, 0.0))


def own_part_kernel(wanted, before_ref, field_ref, high_ref, low_ref, *refs):
    own_ref, moments_ref = refs[-2:]

    @pl.when(is_odd() if wanted else jnp.logical_not(is_odd()))
    def _():
        own_kernel(before_ref, field_ref, high_ref, low_ref, own_ref, moments_ref)


def pair_kernel(own_ref, got_pair_ref, high_up, low_up, base_ref):
    @pl.when(jnp.logical_not(is_odd()))
    def _():
        tile = tile_of(own_ref.shape[1])

        def store(start, part):
            cols = pl.ds(start, tile)
            base_ref[:, cols] = own_ref[:, cols] + part

        forward(stacked(got_pair_ref[...]), high_up, low_up, store)


def even_kernel(base_ref, got_ref, after_ref, field_ref):
    del after_ref

    @pl.when(jnp.logical_not(is_odd()))
    def _():
        field_ref[...] = base_ref[...] + got_ref[...]


def odd_kernel(sign, own_ref, got_pair_ref, got_ref, high_in, low_in, high_up, low_up, after_ref, field_ref, cross_ref):
    del after_ref

    @pl.when(is_odd())
    def _():
        tile = tile_of(own_ref.shape[1])

        def keep(start, part):
            cols = pl.ds(start, tile)
            field_ref[:, cols] = own_ref[:, cols] + sign * (got_pair_ref[:, cols] + part)

        def send(start, part):
            cross_ref[:, pl.ds(start, tile)] = part

        forward(stacked(got_ref[...]), high_up, low_up, keep)
        coupling(stacked(field_ref[...]), high_in, low_in, send)


def couple_even(field_ref, high_in, low_in, pair_ref):
    tile = tile_of(field_ref.shape[1])

    def send(start, part):
        pair_ref[:, pl.ds(start, tile)] = part

    coupling(stacked(field_ref[...]), high_in, low_in, send)


def couple_kernel(field_ref, high_in, low_in, pair_ref):
    @pl.when(jnp.logical_not(is_odd()))
    def _():
        couple_even(field_ref, high_in, low_in, pair_ref)


def merge_kernel(even_ref, odd_ref, field_ref):
    @pl.when(is_odd())
    def _():
        field_ref[...] = odd_ref[...]

    @pl.when(jnp.logical_not(is_odd()))
    def _():
        field_ref[...] = even_ref[...]


def join_kernel(sign, base_ref, got_ref, odd_ref, high_in, low_in, field_ref, pair_ref):
    @pl.when(is_odd())
    def _():
        field_ref[...] = odd_ref[...]
        pair_ref[...] = odd_ref[...]

    @pl.when(jnp.logical_not(is_odd()))
    def _():
        field_ref[...] = base_ref[...] + sign * got_ref[...]
        couple_even(field_ref, high_in, low_in, pair_ref)


def reduce_kernel(field_ref, own_ref, got_pair_ref, got_up_ref, one_ref, two_ref, three_ref, out_ref):
    traits = field_ref.shape[0]
    lower = jnp.where(is_odd(), got_pair_ref[...], got_up_ref[...])
    last = moment(field_ref[...], own_ref[...] + 2.0 * lower)
    lane = lax.broadcasted_iota(jnp.int32, (traits, 128), 1)
    parts = (
        one_ref[:, 0:1],
        two_ref[:, 1:2],
        two_ref[:, 0:1],
        three_ref[:, 1:2],
        three_ref[:, 0:1],
        last,
    )
    table = jnp.zeros((traits, 128), F32)
    for index, part in enumerate(parts):
        table = jnp.where(lane == index, part, table)
    lanes = out_ref.shape[2]
    if lanes > traits:
        table = jnp.concatenate([table, jnp.zeros((lanes - traits, 128), F32)], axis=0)
    rows = jnp.transpose(table)[:MOMENT_ROWS]
    for index in range(out_ref.shape[0]):
        out_ref[index] = rows


def coefficients(moments, shift):
    def inner(left, right):
        total = None
        for i, a in enumerate(left):
            for j, b in enumerate(right):
                term = (a * b) * moments[i + j]
                total = term if total is None else total + term
        return total

    one = jnp.ones_like(shift)
    zero = jnp.zeros_like(shift)
    residual, direction, gain = [one], [one], []
    norm_now = moments[0]
    for step in range(ITERS):
        image = [shift * a + b for a, b in zip(direction + [zero], [zero] + direction)]
        alpha = norm_now / inner(direction, image)
        gain = [a + alpha * b for a, b in zip(gain + [zero], direction)]
        residual = [a - alpha * b for a, b in zip(residual + [zero], image)]
        if step + 1 < ITERS:
            norm_next = inner(residual, residual)
            ratio = norm_next / norm_now
            direction = [a + ratio * b for a, b in zip(residual, direction + [zero])]
            norm_now = norm_next
    return gain, residual


def weights_kernel(table_ref, shrinkage_ref, weights_ref):
    sums = jnp.sum(table_ref[...], axis=0)
    traits, lanes = weights_ref.shape[0], sums.shape[1]
    shift = 1.0 + shrinkage_ref[...]
    moments = [sums[i : i + 1, :traits] for i in range(2 * ITERS)]
    gain, residual = coefficients(moments, shift)
    row = lax.broadcasted_iota(jnp.int32, (lanes, traits), 0)
    table = jnp.zeros((lanes, traits), F32)
    for index, part in enumerate(gain + residual):
        table = jnp.where(row == index, part, table)
    weights_ref[...] = jnp.transpose(table)


def final_kernel(
    weights_ref, start_ref, zero_ref, one_ref, two_ref, own_ref, got_pair_ref, got_down_ref, got_up_ref,
    high_up, low_up, solution_ref, residual_ref, solution, residual, sems,
):
    tile = tile_of(own_ref.shape[1])
    weights = [weights_ref[:, i : i + 1] for i in range(2 * ITERS + 1)]
    gain, rest = weights[:ITERS], weights[ITERS:]
    odd = is_odd()
    zero, one, two = zero_ref[...], one_ref[...], two_ref[...]
    solution[...] = start_ref[...] + gain[0] * zero + gain[1] * one + gain[2] * two
    first = pltpu.make_async_copy(solution, solution_ref, sems.at[0])
    first.start()
    upper = jnp.where(odd, got_down_ref[...], got_pair_ref[...])
    lower = jnp.where(odd, got_pair_ref[...], got_up_ref[...])
    base = rest[0] * zero + rest[1] * one + rest[2] * two + rest[3] * (own_ref[...] + lower)

    def store(start, part):
        residual[:, pl.ds(start, tile)] = base[:, start : start + tile] + rest[3] * part

    forward(stacked(upper), high_up, low_up, store)
    second = pltpu.make_async_copy(residual, residual_ref, sems.at[1])
    second.start()
    first.wait()
    second.wait()


def call(kernel, out, *args, spaces=None, scratch=(), limit=12, aliases=None, keep=True, flops=0):
    spaces = spaces or {}
    places = [spaces.get(i, VMEM) for i in range(len(args))]
    args = [
        arg if place is pltpu.SMEM else pltpu.with_memory_space_constraint(arg, place)
        for arg, place in zip(args, places)
    ]
    make = VMEM if keep else jax.ShapeDtypeStruct
    return pl.pallas_call(
        kernel,
        out_shape=[make(shape, dtype) for shape, dtype in out],
        in_specs=[pl.BlockSpec(memory_space=place) for place in places],
        out_specs=[pl.BlockSpec(memory_space=VMEM if keep else pltpu.HBM) for _ in out],
        scratch_shapes=scratch,
        input_output_aliases=aliases or {},
        cost_estimate=pl.CostEstimate(flops=flops, bytes_accessed=0, transcendentals=0) if flops else None,
        compiler_params=pltpu.CompilerParams(vmem_limit_bytes=limit * 1024 * 1024),
    )(*args)


def on_device(local_block, next_block, shrinkage, marginal, warm_start):
    count = lax.axis_size("snp")
    traits, size = warm_start.shape
    field = ((traits, size), F32)
    table = ((traits, 128), F32)
    matrix = ((size, size), BF16)
    work = 6 * traits * size * size
    copies = (
        pltpu.VMEM((size, size), F32),
        pltpu.VMEM((traits, size), F32),
        pltpu.SemaphoreType.DMA((size // tile_of(size) + 1,)),
    )
    on_chip = [(i, i ^ 1) for i in range(count) if i ^ 1 < count]
    downward = [(i + 1, i) for i in range(1, count - 1, 2)]
    upward = [(i, i + 1) for i in range(1, count - 1, 2)]

    def shift(value, route):
        return lax.ppermute(value, "snp", route)

    def run(kernel, out, *args, **rest):
        return call(kernel, out, *args, **rest)

    hbm = pltpu.HBM
    ridge = shrinkage.reshape(1, traits)
    down = shift(warm_start, downward)
    high_n, low_n, cross = run(
        begin_odd_kernel, [matrix, matrix, field], next_block, warm_start,
        spaces={0: hbm, 1: hbm}, scratch=copies, flops=work,
    )
    high_l, low_l, own, pair = run(
        local_odd_kernel, [matrix, matrix, field, field], local_block, warm_start, cross, flops=work
    )
    up = shift(cross, upward)
    high_n, low_n, pair = run(
        begin_even_kernel, [matrix, matrix, field], next_block, warm_start, high_n, low_n, pair,
        spaces={0: hbm}, scratch=copies[::2], aliases={2: 0, 3: 1, 4: 2}, flops=work,
    )
    got_pair = shift(pair, on_chip)
    rest, high_up, low_up = run(
        prepare_odd_kernel, [field, matrix, matrix],
        own, warm_start, marginal, ridge, high_n, low_n, flops=work,
    )
    odd = functools.partial(odd_kernel, -1.0)
    odd_field, cross = run(odd, [field, field], rest, got_pair, down, high_n, low_n, high_up, low_up, ridge, flops=work)
    next_up = shift(cross, upward)
    high_l, low_l, high_up, low_up, base = run(
        prepare_even_kernel, [matrix, matrix, matrix, matrix, field],
        local_block, warm_start, marginal, ridge, got_pair, high_n, low_n,
        high_l, low_l, high_up, low_up, odd_field,
        aliases={7: 0, 8: 1, 9: 2, 10: 3}, flops=work,
    )
    join = functools.partial(join_kernel, -1.0)
    merged, pair = run(join, [field, field], base, up, odd_field, high_n, low_n, flops=work)
    up = next_up
    fields, tables = [merged], []
    odd, join = functools.partial(odd_kernel, 1.0), functools.partial(join_kernel, 1.0)
    for step in range(2, ITERS + 2):
        got_pair = shift(pair, on_chip)
        if step % 2 == 0:
            down = shift(merged, downward)
        before = fields[-2:-1]
        kernel = own_kernel if before else functools.partial(own_kernel, None)
        if step == 3:
            inputs = (*before, merged, high_l, low_l)
            own, part = run(functools.partial(own_part_kernel, False), [field, table], *inputs, flops=work)
            own, part = run(
                functools.partial(own_part_kernel, True), [field, table], *inputs, own, part,
                aliases={4: 0, 5: 1}, flops=work,
            )
        else:
            own, part = run(kernel, [field, table], *before, merged, high_l, low_l, flops=work)
        tables.append(part)
        if step > ITERS:
            break
        (base,) = run(pair_kernel, [field], own, got_pair, high_up, low_up, flops=work)
        if step % 2 == 0:
            (even_field,) = run(even_kernel, [field], base, up, ridge, flops=work)
            next_down = shift(even_field, downward)
            (early,) = run(couple_kernel, [field], even_field, high_n, low_n, flops=work)
            got_early = shift(early, on_chip)
            odd_field, cross = run(
                odd, [field, field],
                own, got_pair, down, high_n, low_n, high_up, low_up, even_field, flops=work,
            )
            up = shift(cross, upward)
            down = next_down
            (merged,) = run(merge_kernel, [field], even_field, odd_field, flops=work)
            pair = merged
        else:
            odd_field, cross = run(
                odd, [field, field],
                own, got_early, down, high_n, low_n, high_up, low_up, own, flops=work,
            )
            next_up = shift(cross, upward)
            merged, pair = run(join, [field, field], base, up, odd_field, high_n, low_n, flops=work)
            up = next_up
        fields.append(merged)
    lanes = -(-traits // 128) * 128
    (moments,) = run(reduce_kernel, [((count, MOMENT_ROWS, lanes), F32)], fields[-1], own, got_pair, up, *tables)
    moments = lax.all_to_all(moments, "snp", 0, 0)
    (weights,) = run(weights_kernel, [table], moments, ridge)
    return tuple(
        run(
            final_kernel, [field, field],
            weights, warm_start, *fields, own, got_pair, down, up, high_up, low_up,
            keep=False,
            scratch=(pltpu.VMEM((traits, size), F32), pltpu.VMEM((traits, size), F32), pltpu.SemaphoreType.DMA((2,))),
        )
    )


def solution(mesh):
    return jax.shard_map(
        on_device,
        mesh=mesh,
        in_specs=(
            P(("parts", "snp"), None),
            P(("parts", "snp"), None),
            P(),
            P(None, ("parts", "snp")),
            P(None, ("parts", "snp")),
        ),
        out_specs=(P(None, ("parts", "snp")), P(None, ("parts", "snp"))),
        check_vma=False,
    )
```
